32 devices in a mesh: ep: 8 (over z, x), rep: 4 (over y, core).
Axes of the slice: x: 2, y: 2, z: 4, core: 2. Of those that a mesh axis runs over, the one named last changes fastest.
Arguments:
- tension: float32 [4096, 512], P(('rep', 'ep')), parts along dimension 0, may hold values from -6 to 6
- tile_dest: int32 [4096], P(('rep', 'ep')), parts along dimension 0, may hold values from 0 to 1023, as said below
- restriction: float32 [8, 64], replicated, may hold values from -0.75 to 0.75
- elem_block: int32 [32768], P(('rep', 'ep')), parts along dimension 0, may hold values from 0 to 1023
- shared_own: int32 [8192], P(('rep', 'ep')), parts along dimension 0, may hold values from 0 to 1023, as said below
- shared_send: int32 [8192], P(('rep', 'ep')), parts along dimension 0, may hold values from 0 to 1023
Outputs:
- quadrature: float32 [8, 32768], P(None, ('rep', 'ep')), parts along dimension 1
The draws below stay inside these ranges and needn't reach their ends.
There are 4 independent parts, one for each index of `rep`. The reference program is written for one: setup_inputs(seed, part) draws one part's arguments, and reference() takes and returns one part's arrays. A program takes and returns all parts, laid end to end along the dimension named above; an argument that names none is the same for every part. Nothing has to cross between parts.
Inputs may be any that keep to these rules, and one draw needn't show every extreme that they name: `tile_dest`: A permutation of the tile positions. The 128 entries of one device name, for each device's block of 128 positions, either exactly 32 positions in it or none. `shared_own`: the 256 entries of one device are distinct.
All inputs are finite; a program needn't handle non-finite values.
Results may differ from the reference program's by a relative error of at most 0.00007.
Values sent between devices are 32-bit elements; how exact they have to be, the bound alone decides.
A program may use at most 64 MiB of HBM per device.

```python
import jax
import jax.numpy as jnp
from jax import lax

TILE_NODES = 512
ELEM_NODES = 64
QUAD = 8
TILE_DEV = 128
SHARED = 256
BLOCKS = 8
CAP = 32
TILES = 1024
ELEM_DEV = 1024
ELEMENTS = 8192
N_EP = 8


def draw_tile_dest(key, part):
    key_one, key_two, key_three, key_four = jax.random.split(key, 4)
    sigma = jax.random.permutation(key_one, N_EP).astype(jnp.int32)
    tau = jax.random.permutation(key_two, N_EP).astype(jnp.int32)
    linked = ((sigma[:, None] + tau[None, :]) % 2 == 0).astype(jnp.int32)
    half_ep = N_EP // 2
    chosen = jnp.argsort(1 - linked, axis=1, stable=True)[:, :half_ep].astype(jnp.int32)
    offsets = (jnp.cumsum(linked, axis=0) - linked) * CAP
    slot_ids = jnp.arange(TILE_DEV, dtype=jnp.int32)
    dst_of = chosen[:, slot_ids // CAP]
    local_pos = jnp.take_along_axis(offsets, dst_of, axis=1) + (slot_ids % CAP)[None, :]
    shuffle_dst = jax.vmap(lambda sub: jax.random.permutation(sub, TILE_DEV))(jax.random.split(key_three, N_EP)).astype(jnp.int32)
    final_pos = shuffle_dst[dst_of, local_pos]
    global_dest = dst_of * TILE_DEV + final_pos
    shuffle_src = jax.vmap(lambda sub: jax.random.permutation(sub, TILE_DEV))(jax.random.split(key_four, N_EP)).astype(jnp.int32)
    dest = jnp.take_along_axis(global_dest, shuffle_src, axis=1)
    return dest.reshape(TILES).astype(jnp.int32)


def draw_shared_own(key, part):
    orders = jax.vmap(lambda sub: jax.random.permutation(sub, ELEM_DEV))(jax.random.split(jax.random.fold_in(key, 7), N_EP))
    return orders[:, :SHARED].reshape(N_EP * SHARED).astype(jnp.int32)


def touch_ends(entries, own_key, least, top_value):
    longest = entries.shape.index(max(entries.shape))
    spots = []
    for shift in (0, 1):
        where = [jax.random.randint(jax.random.fold_in(own_key, axis), (), 0, length) for axis, length in enumerate(entries.shape)]
        where[longest] = (where[longest] + shift) % entries.shape[longest]
        spots.append(tuple(where))
    return entries.at[spots[0]].set(least).at[spots[1]].set(top_value)


def block_scale(key, extent, pieces, low, largest):
    level = 1.0
    for dim, parts in pieces:
        heights = jax.random.uniform(jax.random.fold_in(jax.random.fold_in(key, 6), dim), (parts,), jnp.float32, low / len(pieces), largest / len(pieces))
        level = level * jnp.repeat(jnp.exp(heights), extent[dim] // parts).reshape((-1,) + (1,) * (len(extent) - 1 - dim))
    return level


def centred(key, extent, width, reach, cuts=(), held_as=jnp.bfloat16):
    factor_of = block_scale(key, extent, cuts, -0.22, 0.18) if cuts else 1.0
    values = jax.random.normal(key, extent, jnp.float32) * width * factor_of
    return jnp.minimum(jnp.maximum(values, -reach), reach).astype(held_as)


def setup_inputs(seed: int = 0, part: int = 0) -> dict:
    arg_keys = jax.random.split(jax.random.key(seed), 7)
    part_keys = jax.random.split(jax.random.fold_in(arg_keys[6], part), 7)
    tension = centred(part_keys[0], (TILES, TILE_NODES), 1.0, 6.0, ((0, 8),), jnp.float32)
    tile_dest = draw_tile_dest(jax.random.fold_in(jax.random.fold_in(arg_keys[6], part), 71), part)
    restriction = centred(arg_keys[2], (QUAD, ELEM_NODES), ELEM_NODES ** -0.5, 0.75, (), jnp.float32)
    elem_block = touch_ends(jax.random.randint(part_keys[3], (ELEMENTS,), 0, ELEM_DEV), jax.random.fold_in(part_keys[3], 1), 0, ELEM_DEV - 1).astype(jnp.int32)
    shared_own = draw_shared_own(jax.random.fold_in(jax.random.fold_in(arg_keys[6], part), 71), part)
    shared_send = touch_ends(jax.random.randint(part_keys[5], (N_EP * SHARED,), 0, ELEM_DEV), jax.random.fold_in(part_keys[5], 1), 0, ELEM_DEV - 1).astype(jnp.int32)
    return {"tension": tension, "tile_dest": tile_dest, "restriction": restriction, "elem_block": elem_block, "shared_own": shared_own, "shared_send": shared_send}


def reference(tension, tile_dest, restriction, elem_block, shared_own, shared_send):
    placed = jnp.zeros_like(tension).at[tile_dest].set(tension)
    blocks = placed.reshape(TILES * BLOCKS, ELEM_NODES)
    owner_dev = jnp.arange(ELEMENTS, dtype=jnp.int32) // ELEM_DEV
    source = (owner_dev * ELEM_DEV + elem_block).astype(jnp.int32)
    quad_values = jnp.dot(blocks[source], restriction.T, precision=lax.Precision.HIGHEST, preferred_element_type=jnp.float32)
    device = jnp.arange(N_EP * SHARED, dtype=jnp.int32) // SHARED
    next_dev = (device + 1) % N_EP
    next_send = jnp.roll(shared_send, -SHARED)
    own_rows = (device * ELEM_DEV + shared_own).astype(jnp.int32)
    ghost_rows = (next_dev * ELEM_DEV + next_send).astype(jnp.int32)
    mixed = 0.5 * (quad_values[own_rows] + quad_values[ghost_rows])
    averaged = quad_values.at[own_rows].set(mixed)
    return averaged.T
```

```python
import functools

import jax
import jax.numpy as jnp
from jax import lax
from jax.experimental import pallas as pl
from jax.experimental.pallas import tpu as pltpu
from jax.sharding import PartitionSpec as P

F32 = jnp.float32
BF16 = jnp.bfloat16
I32 = jnp.int32
MINOR = (((1,), (1,)), ((), ()))
DEPTH = 256


def iota(shape, dim):
    return lax.broadcasted_iota(I32, shape, dim)


def pieces(x):
    high = x.astype(BF16)
    return high, (x - high.astype(F32)).astype(BF16)


def onehot(x):
    return x.astype(F32).astype(BF16)


def minor_dot(a, b):
    return lax.dot_general(a, b, MINOR, preferred_element_type=F32)


def lanes_of(x, index):
    return jnp.take_along_axis(x, index, axis=1, mode="promise_in_bounds")


def layout(n, tiles, nodal, nodes):
    cap = 2 * tiles // n
    blocks = nodal // nodes
    groups = min(tiles // cap, blocks)
    return cap, blocks, groups, blocks // groups


def kernel(n, *refs):
    given, out, held = refs[:6], refs[6], refs[7:13]
    outbox, inbox, meta_out, meta_in, ghost_out, ghost_in, load_sem, pair_sem = refs[13:]
    dest, send, block, restriction, own, tension = held
    me = lax.axis_index("ep")
    tiles = tension.shape[0]
    quad, nodes = restriction.shape
    cap, blocks, groups, vectors = layout(n, tiles, tension.shape[1], nodes)
    rows_e = block.shape[0]
    halves = own.shape[0]
    wide = tiles * halves
    slots = n * cap
    cuts = tension.shape[1] // DEPTH

    small = [pltpu.make_async_copy(a, b, load_sem.at[i]) for i, (a, b) in enumerate(zip(given[:5], held[:5]))]
    columns = [
        pltpu.make_async_copy(
            given[5].at[:, c * DEPTH : (c + 1) * DEPTH],
            tension.at[:, c * DEPTH : (c + 1) * DEPTH],
            load_sem.at[5 + c],
        )
        for c in range(cuts)
    ]
    for load in small[:1] + columns + small[1:]:
        load.start()

    barrier = pltpu.get_barrier_semaphore()
    for k in range(1, n):
        pl.semaphore_signal(barrier, inc=1, device_id={"ep": lax.rem(me + n - k, n)})

    def remote(src, dst, sem, peer):
        return pltpu.make_async_remote_copy(
            src_ref=src, dst_ref=dst, send_sem=pair_sem.at[sem], recv_sem=pair_sem.at[sem + 1], device_id={"ep": peer}
        )

    small[0].wait()
    place = dest[...]
    target = lax.div(place, tiles)
    to_peer = (jnp.broadcast_to(target, (n, tiles)) == iota((n, tiles), 0)).astype(F32)
    earlier = onehot(iota((tiles, tiles), 0) < iota((tiles, tiles), 1))
    before = jnp.dot(to_peer.astype(BF16), earlier, preferred_element_type=F32)
    rank = jnp.sum(before * to_peer, axis=0, keepdims=True).astype(I32)
    at_rank = onehot(jnp.broadcast_to(rank, (tiles, tiles)) == lax.rem(iota((tiles, tiles), 0), cap))
    position = (lax.rem(place, tiles) + 1).astype(F32)
    wanted = jnp.concatenate([to_peer * iota((n, tiles), 1).astype(F32), to_peer * position], axis=0)
    wanted = minor_dot(wanted.astype(BF16), at_rank)
    tile_of, where_to = wanted[:n].astype(I32), wanted[n:]
    for p in range(n):
        meta_out[p, 0:1, :] = where_to[p : p + 1]
        meta_out[(p + n - 1) % n, 1:2, :] = where_to[p : p + 1]

    small[3].wait()
    full = (DEPTH // nodes * quad, DEPTH)
    weight = jnp.concatenate([restriction[...]] * (DEPTH // nodes), axis=1)
    weight = jnp.concatenate([weight] * (DEPTH // nodes), axis=0)
    weight = jnp.where(lax.div(iota(full, 0), quad) == lax.div(iota(full, 1), nodes), weight, 0.0)
    weight = jnp.concatenate(pieces(weight), axis=0)

    small[1].wait()
    small[2].wait()
    for h in range(halves):
        want = jnp.broadcast_to(send[h : h + 1, :], (rows_e, tiles))
        got = lanes_of(block[...], lax.rem(want, tiles))
        ghost_out[h : h + 1, :] = jnp.sum(
            jnp.where(lax.div(want, tiles) == iota((rows_e, tiles), 0), got, 0), axis=0, keepdims=True
        )

    def pack():
        local = []
        for c in range(cuts):
            columns[c].wait()
            both = jnp.concatenate(pieces(tension[:, c * DEPTH : (c + 1) * DEPTH]), axis=0)
            part = minor_dot(weight, both)
            local.append(part[: full[0], :tiles] + (part[: full[0], tiles:] + part[full[0] :, :tiles]))
        local = jnp.concatenate(local, axis=0)
        group = lax.div(iota((quad, tiles), 1), cap)
        for p in range(n):
            index = jnp.broadcast_to(tile_of[p : p + 1], (quad, tiles))
            for v in range(vectors):
                low = v * groups * quad
                got = lanes_of(local[low : low + quad], index)
                for g in range(1, groups):
                    low = (v * groups + g) * quad
                    got = jnp.where(group == g, lanes_of(local[low : low + quad], index), got)
                outbox[p, v * quad : (v + 1) * quad, :] = got
                outbox[(p + n - 1) % n, (vectors + v) * quad : (vectors + v + 1) * quad, :] = got

    if not EARLY:
        pack()
    pl.semaphore_wait(barrier, n - 1)
    peers = [lax.rem(me + k, n) for k in range(1, n)]
    for peer in peers:
        remote(meta_out.at[peer], meta_in.at[me], 0, peer).start()
    if not EARLY:
        for peer in peers:
            remote(outbox.at[peer], inbox.at[me], 2, peer).start()
    ghosts = remote(ghost_out, ghost_in, 4, lax.rem(me + n - 1, n))
    ghosts.start()
    if EARLY:
        pack()
        for peer in peers:
            remote(outbox.at[peer], inbox.at[me], 2, peer).start()
    meta_in[me] = meta_out[me]
    inbox[me] = outbox[me]

    small[4].wait()
    owned = jnp.concatenate([own[h : h + 1, :] for h in range(halves)], axis=1)
    entry = (iota((rows_e, wide), 1) + 1).astype(F32)
    entry = jnp.where(
        jnp.broadcast_to(lax.div(owned, tiles), (rows_e, wide)) == iota((rows_e, wide), 0), entry, 0.0
    ).astype(BF16)
    column = jnp.broadcast_to(lax.rem(owned, tiles), (tiles, wide)) == iota((tiles, wide), 0)
    shared = minor_dot(entry, onehot(column)).astype(I32)

    def whole(a, b, sem):
        return remote(a.at[pl.ds(0, n - 1)], b.at[pl.ds(0, n - 1)], sem, lax.rem(me + 1, n))

    ghosts.wait_recv()
    metas = whole(meta_out, meta_in, 0)
    metas.wait_recv()
    per = tiles // cap
    lane = lax.div(iota((1, tiles), 1), cap)
    hits = []
    for kind in range(2):
        parts = []
        for h in range(slots // tiles):
            pos = jnp.zeros((1, tiles), F32)
            for s in range(per):
                pos = jnp.where(lane == s, meta_in[h * per + s, kind : kind + 1, :], pos)
            pos = jnp.broadcast_to(pos.astype(I32), (tiles, tiles))
            parts.append(onehot(pos == iota((tiles, tiles), 0) + 1))
        hits.append(jnp.concatenate(parts, axis=1))
    number = iota((rows_e, slots), 1).astype(F32).astype(BF16)
    came_in = minor_dot(number, jnp.concatenate(hits, axis=0)).astype(I32)

    def find(index, table):
        slot = lanes_of(table, lax.div(index, blocks))
        part = lax.rem(index, blocks)
        return (
            lax.rem(part, groups) * cap + lax.rem(slot, cap),
            lax.div(slot, cap) * vectors + lax.div(part, groups),
        )

    which = jnp.maximum(shared - 1, 0)
    other = jnp.zeros((rows_e, tiles), I32)
    for h in range(halves):
        row = jnp.broadcast_to(ghost_in[h : h + 1, :], (rows_e, tiles))
        other = jnp.where(lax.div(which, tiles) == h, lanes_of(row, lax.rem(which, tiles)), other)
    own_lane, own_vector = find(block[...], came_in[:, :tiles])
    ghost_lane, ghost_vector = find(other, came_in[:, tiles:])

    data = whole(outbox, inbox, 2)
    data.wait_recv()

    def spread(x, r):
        return jnp.broadcast_to(x[r : r + 1, :], (quad, tiles))

    def take(r, lane_at, vector_at, base):
        index, vector = spread(lane_at, r), spread(vector_at, r)

        def step(s, got):
            for v in range(vectors):
                low = base + v * quad
                here = lanes_of(inbox[s, low : low + quad, :], index)
                got = jnp.where(vector == s * vectors + v, here, got)
            return got

        return lax.fori_loop(0, n, step, jnp.zeros((quad, tiles), F32), unroll=n <= 16)

    for r in range(rows_e):
        mine = take(r, own_lane, own_vector, 0)
        theirs = take(r, ghost_lane, ghost_vector, vectors * quad)
        out[:, r * tiles : (r + 1) * tiles] = jnp.where(spread(shared, r) > 0, 0.5 * (mine + theirs), mine)

    ghosts.wait_send()
    metas.wait_send()
    data.wait_send()


EARLY = True


def per_device(tension, tile_dest, restriction, elem_block, shared_own, shared_send):
    n = lax.axis_size("ep")
    tiles = tension.shape[0]
    quad, nodes = restriction.shape
    vectors = layout(n, tiles, tension.shape[1], nodes)[3]
    halves = shared_own.shape[0] // tiles
    given = (
        tile_dest.reshape(1, tiles),
        shared_send.reshape(halves, tiles),
        elem_block.reshape(-1, tiles),
        restriction,
        shared_own.reshape(halves, tiles),
        tension,
    )
    return pl.pallas_call(
        functools.partial(kernel, n),
        out_shape=jax.ShapeDtypeStruct((quad, elem_block.shape[0]), F32),
        in_specs=[pl.BlockSpec(memory_space=pltpu.HBM)] * 6,
        out_specs=pl.BlockSpec(memory_space=pltpu.VMEM),
        scratch_shapes=[pltpu.VMEM(a.shape, a.dtype) for a in given]
        + [
            pltpu.VMEM((n, 2 * vectors * quad, tiles), F32),
            pltpu.VMEM((n, 2 * vectors * quad, tiles), F32),
            pltpu.VMEM((n, 2, tiles), F32),
            pltpu.VMEM((n, 2, tiles), F32),
            pltpu.VMEM((halves, tiles), I32),
            pltpu.VMEM((halves, tiles), I32),
            pltpu.SemaphoreType.DMA((5 + tension.shape[1] // DEPTH,)),
            pltpu.SemaphoreType.DMA((6,)),
        ],
        compiler_params=pltpu.CompilerParams(
            collective_id=0, has_side_effects=True, vmem_limit_bytes=16 * 2**20
        ),
    )(*[pltpu.with_memory_space_constraint(a, pltpu.HBM) for a in given])


def solution(mesh):
    return jax.shard_map(
        per_device,
        mesh=mesh,
        in_specs=(
            P(("rep", "ep"), None),
            P(("rep", "ep")),
            P(),
            P(("rep", "ep")),
            P(("rep", "ep")),
            P(("rep", "ep")),
        ),
        out_specs=P(None, ("rep", "ep")),
        check_vma=False,
    )
```

```python
import functools

import jax
import jax.numpy as jnp
from jax import lax
from jax.experimental import pallas as pl
from jax.experimental.pallas import tpu as pltpu
from jax.sharding import PartitionSpec as P

F32 = jnp.float32
BF16 = jnp.bfloat16
I32 = jnp.int32
MINOR = (((1,), (1,)), ((), ()))
DEPTH = 256


def iota(shape, dim):
    return lax.broadcasted_iota(I32, shape, dim)


def pieces(x):
    high = x.astype(BF16)
    return high, (x - high.astype(F32)).astype(BF16)


def onehot(x):
    return x.astype(F32).astype(BF16)


def minor_dot(a, b):
    return lax.dot_general(a, b, MINOR, preferred_element_type=F32)


def lanes_of(x, index):
    return jnp.take_along_axis(x, index, axis=1, mode="promise_in_bounds")


def layout(n, tiles, nodal, nodes):
    cap = 2 * tiles // n
    blocks = nodal // nodes
    groups = min(tiles // cap, blocks)
    return cap, blocks, groups, blocks // groups


def stages(n):
    return (n // 2 + 1, n - 1)


def kernel(n, *refs):
    given, out, held = refs[:6], refs[6], refs[7:13]
    outbox, inbox, meta_out, meta_in, ghost_out, ghost_in, load_sem, pair_sem, entered = refs[13:]
    dest, send, block, restriction, own, tension = held
    me = lax.axis_index("ep")
    tiles = tension.shape[0]
    quad, nodes = restriction.shape
    cap, blocks, groups, vectors = layout(n, tiles, tension.shape[1], nodes)
    rows_e = block.shape[0]
    halves = own.shape[0]
    wide = tiles * halves
    slots = n * cap
    cuts = tension.shape[1] // DEPTH

    small = [pltpu.make_async_copy(a, b, load_sem.at[i]) for i, (a, b) in enumerate(zip(given[:5], held[:5]))]
    columns = [
        pltpu.make_async_copy(
            given[5].at[:, c * DEPTH : (c + 1) * DEPTH],
            tension.at[:, c * DEPTH : (c + 1) * DEPTH],
            load_sem.at[5 + c],
        )
        for c in range(cuts)
    ]
    for load in small[:1] + columns + small[1:]:
        load.start()

    barrier = pltpu.get_barrier_semaphore()

    def each(first, last, step):
        lax.fori_loop(first, last, lambda p, _: (step(p), 0)[1], 0)

    each(me + 1, n, lambda p: pl.semaphore_signal(barrier, inc=1, device_id={"ep": p}))

    last = n - 1
    edges = stages(n)
    parts_of = [range(a, b) for a, b in zip((0,) + edges, edges + (n,))]
    count = len(parts_of)
    my_part = sum((me >= edge).astype(I32) for edge in edges)

    def remote(src, dst, sent, got, peer):
        return pltpu.make_async_remote_copy(
            src_ref=src, dst_ref=dst, send_sem=pair_sem.at[sent], recv_sem=pair_sem.at[got], device_id={"ep": peer}
        )

    def send_meta(p):
        remote(meta_out.at[p], meta_in.at[me], 0, 4 + my_part, p).start()

    def send_data(p):
        remote(outbox.at[p], inbox.at[me], 1, 4 + count + my_part, p).start()

    def send_both(p):
        send_meta(p)
        send_data(p)

    def several(a, b, many, sent, got):
        return remote(a.at[pl.ds(0, many)], b.at[pl.ds(0, many)], sent, got, lax.rem(me + 1, n))

    ghosts = remote(ghost_out, ghost_in, 2, 3, lax.rem(me + last, n))

    @pl.when(me > 0)
    def _():
        pl.semaphore_wait(barrier, me)

    each(0, me, lambda p: pl.semaphore_signal(entered.at[me], inc=1, device_id={"ep": p}))

    for i in (0, 3, 1, 2):
        small[i].wait()
    place = dest[...]
    target = lax.div(place, tiles)
    to_peer = (jnp.broadcast_to(target, (n, tiles)) == iota((n, tiles), 0)).astype(F32)
    earlier = onehot(iota((tiles, tiles), 0) < iota((tiles, tiles), 1))
    before = jnp.dot(to_peer.astype(BF16), earlier, preferred_element_type=F32)
    rank = jnp.sum(before * to_peer, axis=0, keepdims=True).astype(I32)
    at_rank = onehot(jnp.broadcast_to(rank, (tiles, tiles)) == lax.rem(iota((tiles, tiles), 0), cap))
    position = (lax.rem(place, tiles) + 1).astype(F32)
    wanted = jnp.concatenate([to_peer * iota((n, tiles), 1).astype(F32), to_peer * position], axis=0)
    wanted = minor_dot(wanted.astype(BF16), at_rank)
    tile_of, where_to = wanted[:n].astype(I32), wanted[n:]
    for p in range(n):
        meta_out[p, 0:1, :] = where_to[p : p + 1]
        meta_out[(p + n - 1) % n, 1:2, :] = where_to[p : p + 1]

    full = (DEPTH // nodes * quad, DEPTH)
    weight = jnp.concatenate([restriction[...]] * (DEPTH // nodes), axis=1)
    weight = jnp.concatenate([weight] * (DEPTH // nodes), axis=0)
    weight = jnp.where(lax.div(iota(full, 0), quad) == lax.div(iota(full, 1), nodes), weight, 0.0)
    weight = jnp.concatenate(pieces(weight), axis=0)

    for h in range(halves):
        want = jnp.broadcast_to(send[h : h + 1, :], (rows_e, tiles))
        got = lanes_of(block[...], lax.rem(want, tiles))
        ghost_out[h : h + 1, :] = jnp.sum(
            jnp.where(lax.div(want, tiles) == iota((rows_e, tiles), 0), got, 0), axis=0, keepdims=True
        )

    def pack():
        for load in columns:
            load.wait()
        local = []
        for c in range(cuts):
            both = jnp.concatenate(pieces(tension[:, c * DEPTH : (c + 1) * DEPTH]), axis=0)
            part = minor_dot(weight, both)
            local.append(part[: full[0], :tiles] + (part[: full[0], tiles:] + part[full[0] :, :tiles]))
        local = jnp.concatenate(local, axis=0)
        group = lax.div(iota((quad, tiles), 1), cap)
        for p in range(n):
            index = jnp.broadcast_to(tile_of[p : p + 1], (quad, tiles))
            for v in range(vectors):
                low = v * groups * quad
                got = lanes_of(local[low : low + quad], index)
                for g in range(1, groups):
                    low = (v * groups + g) * quad
                    got = jnp.where(group == g, lanes_of(local[low : low + quad], index), got)
                outbox[p, v * quad : (v + 1) * quad, :] = got
                outbox[(p + n - 1) % n, (vectors + v) * quad : (vectors + v + 1) * quad, :] = got

    @pl.when(me > 0)
    def _():
        send_meta(0)
        ghosts.start()

    pack()

    @pl.when(me > 0)
    def _():
        send_data(0)

    each(1, me, send_both)

    def up(p):
        pl.semaphore_wait(entered.at[p], 1)
        send_both(p)

    each(me + 1, n, up)

    @pl.when(me == 0)
    def _():
        ghosts.start()

    meta_in[me] = meta_out[me]
    inbox[me] = outbox[me]

    small[4].wait()
    owned = jnp.concatenate([own[h : h + 1, :] for h in range(halves)], axis=1)
    entry = (iota((rows_e, wide), 1) + 1).astype(F32)
    entry = jnp.where(
        jnp.broadcast_to(lax.div(owned, tiles), (rows_e, wide)) == iota((rows_e, wide), 0), entry, 0.0
    ).astype(BF16)
    column = jnp.broadcast_to(lax.rem(owned, tiles), (tiles, wide)) == iota((tiles, wide), 0)
    shared = minor_dot(entry, onehot(column)).astype(I32)

    which = jnp.maximum(shared - 1, 0)
    ghosts.wait_recv()
    other = jnp.zeros((rows_e, tiles), I32)
    for h in range(halves):
        row = jnp.broadcast_to(ghost_in[h : h + 1, :], (rows_e, tiles))
        other = jnp.where(lax.div(which, tiles) == h, lanes_of(row, lax.rem(which, tiles)), other)

    per = tiles // cap
    lane = lax.div(iota((1, tiles), 1), cap)

    def came_in(sources):
        first = sources[0] // per
        spans = range(first, sources[-1] // per + 1)
        hits = []
        for kind in range(2):
            parts = []
            for h in spans:
                pos = jnp.zeros((1, tiles), F32)
                for s in range(per):
                    if h * per + s in sources:
                        pos = jnp.where(lane == s, meta_in[h * per + s, kind : kind + 1, :], pos)
                pos = jnp.broadcast_to(pos.astype(I32), (tiles, tiles))
                parts.append(onehot(pos == iota((tiles, tiles), 0) + 1))
            hits.append(jnp.concatenate(parts, axis=1))
        number = iota((rows_e, len(spans) * tiles), 1) + (first * tiles + 1)
        return minor_dot(number.astype(F32).astype(BF16), jnp.concatenate(hits, axis=0)).astype(I32)

    def find(index, table):
        slot = lanes_of(table, lax.div(index, blocks))
        part = lax.rem(index, blocks)
        there = jnp.maximum(slot - 1, 0)
        vector = lax.div(there, cap) * vectors + lax.div(part, groups)
        return lax.rem(part, groups) * cap + lax.rem(there, cap), jnp.where(slot > 0, vector, -1)

    def find_all(sources):
        table = came_in(sources)
        return find(block[...], table[:, :tiles]) + find(other, table[:, tiles:])

    def spread(x, r):
        return jnp.broadcast_to(x[r : r + 1, :], (quad, tiles))

    def take(r, lane_at, vector_at, base, first, end, got):
        index, vector = spread(lane_at, r), spread(vector_at, r)

        def step(s, got):
            for v in range(vectors):
                low = base + v * quad
                here = lanes_of(inbox[s, low : low + quad, :], index)
                got = jnp.where(vector == s * vectors + v, here, got)
            return got

        return lax.fori_loop(first, end, step, got, unroll=end - first <= 16)

    def take_all(found, first, end, mine, theirs):
        for r in range(rows_e):
            mine[r] = take(r, found[0], found[1], 0, first, end, mine[r])
            theirs[r] = take(r, found[2], found[3], vectors * quad, first, end, theirs[r])

    def arrived(a, b, sent, got, sources):
        ours = (me >= sources[0]) & (me <= sources[-1])
        for many, there in ((len(sources) - 1, ours), (len(sources), jnp.logical_not(ours))):
            if many:

                @pl.when(there)
                def _():
                    several(a, b, many, sent, got).wait_recv()

    mine = [jnp.zeros((quad, tiles), F32)] * rows_e
    theirs = [jnp.zeros((quad, tiles), F32)] * rows_e
    for i, sources in enumerate(parts_of):
        arrived(meta_out, meta_in, 0, 4 + i, sources)
        found = find_all(sources)
        arrived(outbox, inbox, 1, 4 + count + i, sources)
        take_all(found, sources[0], sources[-1] + 1, mine, theirs)
    for r in range(rows_e):
        out[:, r * tiles : (r + 1) * tiles] = jnp.where(
            spread(shared, r) > 0, 0.5 * (mine[r] + theirs[r]), mine[r]
        )

    ghosts.wait_send()
    several(meta_out, meta_in, last, 0, 4).wait_send()
    several(outbox, inbox, last, 1, 4 + count).wait_send()


def per_device(tension, tile_dest, restriction, elem_block, shared_own, shared_send):
    n = lax.axis_size("ep")
    tiles = tension.shape[0]
    quad, nodes = restriction.shape
    vectors = layout(n, tiles, tension.shape[1], nodes)[3]
    halves = shared_own.shape[0] // tiles
    given = (
        tile_dest.reshape(1, tiles),
        shared_send.reshape(halves, tiles),
        elem_block.reshape(-1, tiles),
        restriction,
        shared_own.reshape(halves, tiles),
        tension,
    )
    return pl.pallas_call(
        functools.partial(kernel, n),
        out_shape=jax.ShapeDtypeStruct((quad, elem_block.shape[0]), F32),
        in_specs=[pl.BlockSpec(memory_space=pltpu.HBM)] * 6,
        out_specs=pl.BlockSpec(memory_space=pltpu.VMEM),
        scratch_shapes=[pltpu.VMEM(a.shape, a.dtype) for a in given]
        + [
            pltpu.VMEM((n, 2 * vectors * quad, tiles), F32),
            pltpu.VMEM((n, 2 * vectors * quad, tiles), F32),
            pltpu.VMEM((n, 2, tiles), F32),
            pltpu.VMEM((n, 2, tiles), F32),
            pltpu.VMEM((halves, tiles), I32),
            pltpu.VMEM((halves, tiles), I32),
            pltpu.SemaphoreType.DMA((5 + tension.shape[1] // DEPTH,)),
            pltpu.SemaphoreType.DMA((4 + 2 * (len(stages(n)) + 1),)),
            pltpu.SemaphoreType.REGULAR((n,)),
        ],
        compiler_params=pltpu.CompilerParams(
            collective_id=0, has_side_effects=True, vmem_limit_bytes=16 * 2**20
        ),
    )(*[pltpu.with_memory_space_constraint(a, pltpu.HBM) for a in given])


def solution(mesh):
    return jax.shard_map(
        per_device,
        mesh=mesh,
        in_specs=(
            P(("rep", "ep"), None),
            P(("rep", "ep")),
            P(),
            P(("rep", "ep")),
            P(("rep", "ep")),
            P(("rep", "ep")),
        ),
        out_specs=P(None, ("rep", "ep")),
        check_vma=False,
    )
```

```python
import functools

import jax
import jax.numpy as jnp
from jax import lax
from jax.experimental import pallas as pl
from jax.experimental.pallas import tpu as pltpu
from jax.sharding import PartitionSpec as P

F32 = jnp.float32
BF16 = jnp.bfloat16
I32 = jnp.int32
MINOR = (((1,), (1,)), ((), ()))
DEPTH = 256


def iota(shape, dim):
    return lax.broadcasted_iota(I32, shape, dim)


def pieces(x):
    high = x.astype(BF16)
    return high, (x - high.astype(F32)).astype(BF16)


def onehot(x):
    return x.astype(F32).astype(BF16)


def minor_dot(a, b):
    return lax.dot_general(a, b, MINOR, preferred_element_type=F32)


def lanes_of(x, index):
    return jnp.take_along_axis(x, index, axis=1, mode="promise_in_bounds")


def layout(n, tiles, nodal, nodes):
    cap = 2 * tiles // n
    blocks = nodal // nodes
    groups = min(tiles // cap, blocks)
    return cap, blocks, groups, blocks // groups


def stages(n):
    return (n // 2 + 1, n - 1)


def kernel(n, *refs):
    given, out, held = refs[:6], refs[6], refs[7:13]
    outbox, inbox, meta_out, meta_in, ghost_out, ghost_in, load_sem, pair_sem, entered = refs[13:]
    dest, send, block, restriction, own, tension = held
    me = lax.axis_index("ep")
    tiles = tension.shape[0]
    quad, nodes = restriction.shape
    cap, blocks, groups, vectors = layout(n, tiles, tension.shape[1], nodes)
    rows_e = block.shape[0]
    halves = own.shape[0]
    wide = tiles * halves
    slots = n * cap
    cuts = tension.shape[1] // DEPTH

    small = [pltpu.make_async_copy(a, b, load_sem.at[i]) for i, (a, b) in enumerate(zip(given[:5], held[:5]))]
    columns = [
        pltpu.make_async_copy(
            given[5].at[:, c * DEPTH : (c + 1) * DEPTH],
            tension.at[:, c * DEPTH : (c + 1) * DEPTH],
            load_sem.at[5 + c],
        )
        for c in range(cuts)
    ]
    for load in small[:1] + columns + small[1:]:
        load.start()

    barrier = pltpu.get_barrier_semaphore()

    def each(first, last, step):
        lax.fori_loop(first, last, lambda p, _: (step(p), 0)[1], 0)

    each(me + 1, n, lambda p: pl.semaphore_signal(barrier, inc=1, device_id={"ep": p}))

    last = n - 1
    edges = stages(n)
    parts_of = [range(a, b) for a, b in zip((0,) + edges, edges + (n,))]
    count = len(parts_of)
    my_part = sum((me >= edge).astype(I32) for edge in edges)

    def remote(src, dst, sent, got, peer):
        return pltpu.make_async_remote_copy(
            src_ref=src, dst_ref=dst, send_sem=pair_sem.at[sent], recv_sem=pair_sem.at[got], device_id={"ep": peer}
        )

    def send_meta(p):
        remote(meta_out.at[p], meta_in.at[me], 0, 4 + my_part, p).start()

    def send_data(p):
        remote(outbox.at[p], inbox.at[me], 1, 4 + count + my_part, p).start()

    def send_both(p):
        send_meta(p)
        send_data(p)

    def several(a, b, many, sent, got):
        return remote(a.at[pl.ds(0, many)], b.at[pl.ds(0, many)], sent, got, lax.rem(me + 1, n))

    ghosts = remote(ghost_out, ghost_in, 2, 3, lax.rem(me + last, n))

    @pl.when(me > 0)
    def _():
        pl.semaphore_wait(barrier, me)

    each(0, me, lambda p: pl.semaphore_signal(entered.at[me], inc=1, device_id={"ep": p}))

    for i in (0, 3, 1, 2):
        small[i].wait()
    place = dest[...]
    target = lax.div(place, tiles)
    to_peer = (jnp.broadcast_to(target, (n, tiles)) == iota((n, tiles), 0)).astype(F32)
    earlier = onehot(iota((tiles, tiles), 0) < iota((tiles, tiles), 1))
    before = jnp.dot(to_peer.astype(BF16), earlier, preferred_element_type=F32)
    rank = jnp.sum(before * to_peer, axis=0, keepdims=True).astype(I32)
    at_rank = onehot(jnp.broadcast_to(rank, (tiles, tiles)) == lax.rem(iota((tiles, tiles), 0), cap))
    position = (lax.rem(place, tiles) + 1).astype(F32)
    wanted = jnp.concatenate([to_peer * iota((n, tiles), 1).astype(F32), to_peer * position], axis=0)
    wanted = minor_dot(wanted.astype(BF16), at_rank)
    tile_of, where_to = wanted[:n].astype(I32), wanted[n:]
    for p in range(n):
        meta_out[p, 0:1, :] = where_to[p : p + 1]
        meta_out[(p + n - 1) % n, 1:2, :] = where_to[p : p + 1]

    full = (DEPTH // nodes * quad, DEPTH)
    weight = jnp.concatenate([restriction[...]] * (DEPTH // nodes), axis=1)
    weight = jnp.concatenate([weight] * (DEPTH // nodes), axis=0)
    weight = jnp.where(lax.div(iota(full, 0), quad) == lax.div(iota(full, 1), nodes), weight, 0.0)
    weight = jnp.concatenate(pieces(weight), axis=0)

    for h in range(halves):
        want = jnp.broadcast_to(send[h : h + 1, :], (rows_e, tiles))
        got = lanes_of(block[...], lax.rem(want, tiles))
        ghost_out[h : h + 1, :] = jnp.sum(
            jnp.where(lax.div(want, tiles) == iota((rows_e, tiles), 0), got, 0), axis=0, keepdims=True
        )

    @pl.when(me > 0)
    def _():
        send_meta(0)
        ghosts.start()

    for load in columns:
        load.wait()
    local = []
    for c in range(cuts):
        both = jnp.concatenate(pieces(tension[:, c * DEPTH : (c + 1) * DEPTH]), axis=0)
        part = minor_dot(weight, both)
        local.append(part[: full[0], :tiles] + (part[: full[0], tiles:] + part[full[0] :, :tiles]))
    local = jnp.concatenate(local, axis=0)
    group = lax.div(iota((quad, tiles), 1), cap)

    def pack(p):
        index = jnp.broadcast_to(tile_of[p : p + 1], (quad, tiles))
        for v in range(vectors):
            low = v * groups * quad
            got = lanes_of(local[low : low + quad], index)
            for g in range(1, groups):
                low = (v * groups + g) * quad
                got = jnp.where(group == g, lanes_of(local[low : low + quad], index), got)
            outbox[p, v * quad : (v + 1) * quad, :] = got
            outbox[(p + n - 1) % n, (vectors + v) * quad : (vectors + v + 1) * quad, :] = got

    pack(0)
    pack(1)

    @pl.when(me > 0)
    def _():
        send_data(0)

    for p in range(2, n):
        pack(p)
    each(1, me, send_both)

    def up(p):
        pl.semaphore_wait(entered.at[p], 1)
        send_both(p)

    each(me + 1, n, up)

    @pl.when(me == 0)
    def _():
        ghosts.start()

    meta_in[me] = meta_out[me]
    inbox[me] = outbox[me]

    small[4].wait()
    owned = jnp.concatenate([own[h : h + 1, :] for h in range(halves)], axis=1)
    entry = (iota((rows_e, wide), 1) + 1).astype(F32)
    entry = jnp.where(
        jnp.broadcast_to(lax.div(owned, tiles), (rows_e, wide)) == iota((rows_e, wide), 0), entry, 0.0
    ).astype(BF16)
    column = jnp.broadcast_to(lax.rem(owned, tiles), (tiles, wide)) == iota((tiles, wide), 0)
    shared = minor_dot(entry, onehot(column)).astype(I32)

    which = jnp.maximum(shared - 1, 0)
    ghosts.wait_recv()
    other = jnp.zeros((rows_e, tiles), I32)
    for h in range(halves):
        row = jnp.broadcast_to(ghost_in[h : h + 1, :], (rows_e, tiles))
        other = jnp.where(lax.div(which, tiles) == h, lanes_of(row, lax.rem(which, tiles)), other)

    per = tiles // cap
    lane = lax.div(iota((1, tiles), 1), cap)

    def came_in(sources):
        first = sources[0] // per
        spans = range(first, sources[-1] // per + 1)
        hits = []
        for kind in range(2):
            parts = []
            for h in spans:
                pos = jnp.zeros((1, tiles), F32)
                for s in range(per):
                    if h * per + s in sources:
                        pos = jnp.where(lane == s, meta_in[h * per + s, kind : kind + 1, :], pos)
                pos = jnp.broadcast_to(pos.astype(I32), (tiles, tiles))
                parts.append(onehot(pos == iota((tiles, tiles), 0) + 1))
            hits.append(jnp.concatenate(parts, axis=1))
        number = iota((rows_e, len(spans) * tiles), 1) + (first * tiles + 1)
        return minor_dot(number.astype(F32).astype(BF16), jnp.concatenate(hits, axis=0)).astype(I32)

    def find(index, table):
        slot = lanes_of(table, lax.div(index, blocks))
        part = lax.rem(index, blocks)
        there = jnp.maximum(slot - 1, 0)
        vector = lax.div(there, cap) * vectors + lax.div(part, groups)
        return lax.rem(part, groups) * cap + lax.rem(there, cap), jnp.where(slot > 0, vector, -1)

    def find_all(sources):
        table = came_in(sources)
        return find(block[...], table[:, :tiles]) + find(other, table[:, tiles:])

    def spread(x, r):
        return jnp.broadcast_to(x[r : r + 1, :], (quad, tiles))

    def take(r, lane_at, vector_at, base, first, end, got):
        index, vector = spread(lane_at, r), spread(vector_at, r)

        def step(s, got):
            for v in range(vectors):
                low = base + v * quad
                here = lanes_of(inbox[s, low : low + quad, :], index)
                got = jnp.where(vector == s * vectors + v, here, got)
            return got

        return lax.fori_loop(first, end, step, got, unroll=end - first <= 16)

    def take_all(found, first, end, mine, theirs):
        for r in range(rows_e):
            mine[r] = take(r, found[0], found[1], 0, first, end, mine[r])
            theirs[r] = take(r, found[2], found[3], vectors * quad, first, end, theirs[r])

    def arrived(a, b, sent, got, sources):
        ours = (me >= sources[0]) & (me <= sources[-1])
        for many, there in ((len(sources) - 1, ours), (len(sources), jnp.logical_not(ours))):
            if many:

                @pl.when(there)
                def _():
                    several(a, b, many, sent, got).wait_recv()

    mine = [jnp.zeros((quad, tiles), F32)] * rows_e
    theirs = [jnp.zeros((quad, tiles), F32)] * rows_e
    arrived(meta_out, meta_in, 0, 4, parts_of[0])
    found = find_all(parts_of[0])
    for i, sources in enumerate(parts_of):
        arrived(outbox, inbox, 1, 4 + count + i, sources)
        if i + 1 < count:
            arrived(meta_out, meta_in, 0, 5 + i, parts_of[i + 1])
        take_all(found, sources[0], sources[-1] + 1, mine, theirs)
        if i + 1 < count:
            found = find_all(parts_of[i + 1])
    for r in range(rows_e):
        out[:, r * tiles : (r + 1) * tiles] = jnp.where(
            spread(shared, r) > 0, 0.5 * (mine[r] + theirs[r]), mine[r]
        )

    ghosts.wait_send()
    several(meta_out, meta_in, last, 0, 4).wait_send()
    several(outbox, inbox, last, 1, 4 + count).wait_send()


def per_device(tension, tile_dest, restriction, elem_block, shared_own, shared_send):
    n = lax.axis_size("ep")
    tiles = tension.shape[0]
    quad, nodes = restriction.shape
    vectors = layout(n, tiles, tension.shape[1], nodes)[3]
    halves = shared_own.shape[0] // tiles
    given = (
        tile_dest.reshape(1, tiles),
        shared_send.reshape(halves, tiles),
        elem_block.reshape(-1, tiles),
        restriction,
        shared_own.reshape(halves, tiles),
        tension,
    )
    return pl.pallas_call(
        functools.partial(kernel, n),
        out_shape=jax.ShapeDtypeStruct((quad, elem_block.shape[0]), F32),
        in_specs=[pl.BlockSpec(memory_space=pltpu.HBM)] * 6,
        out_specs=pl.BlockSpec(memory_space=pltpu.VMEM),
        scratch_shapes=[pltpu.VMEM(a.shape, a.dtype) for a in given]
        + [
            pltpu.VMEM((n, 2 * vectors * quad, tiles), F32),
            pltpu.VMEM((n, 2 * vectors * quad, tiles), F32),
            pltpu.VMEM((n, 2, tiles), F32),
            pltpu.VMEM((n, 2, tiles), F32),
            pltpu.VMEM((halves, tiles), I32),
            pltpu.VMEM((halves, tiles), I32),
            pltpu.SemaphoreType.DMA((5 + tension.shape[1] // DEPTH,)),
            pltpu.SemaphoreType.DMA((4 + 2 * (len(stages(n)) + 1),)),
            pltpu.SemaphoreType.REGULAR((n,)),
        ],
        compiler_params=pltpu.CompilerParams(
            collective_id=0, has_side_effects=True, vmem_limit_bytes=16 * 2**20
        ),
    )(*[pltpu.with_memory_space_constraint(a, pltpu.HBM) for a in given])


def solution(mesh):
    return jax.shard_map(
        per_device,
        mesh=mesh,
        in_specs=(
            P(("rep", "ep"), None),
            P(("rep", "ep")),
            P(),
            P(("rep", "ep")),
            P(("rep", "ep")),
            P(("rep", "ep")),
        ),
        out_specs=P(None, ("rep", "ep")),
        check_vma=False,
    )
```

```python
import functools

import jax
import jax.numpy as jnp
from jax import lax
from jax.experimental import pallas as pl
from jax.experimental.pallas import tpu as pltpu
from jax.sharding import PartitionSpec as P

F32 = jnp.float32
BF16 = jnp.bfloat16
I32 = jnp.int32
MINOR = (((1,), (1,)), ((), ()))
DEPTH = 256
LOADS = 8


def iota(shape, dim):
    return lax.broadcasted_iota(I32, shape, dim)


def pieces(x):
    high = x.astype(BF16)
    return high, (x - high.astype(F32)).astype(BF16)


def onehot(x):
    return x.astype(F32).astype(BF16)


def minor_dot(a, b):
    return lax.dot_general(a, b, MINOR, preferred_element_type=F32)


def lanes_of(x, index):
    return jnp.take_along_axis(x, index, axis=1, mode="promise_in_bounds")


def layout(n, tiles, nodal, nodes):
    cap = 2 * tiles // n
    blocks = nodal // nodes
    groups = min(tiles // cap, blocks)
    return cap, blocks, groups, blocks // groups


def stages(n):
    return (n // 2 + 1, n - 1)


def kernel(n, *refs):
    given, out, held = refs[:6], refs[6], refs[7:13]
    outbox, inbox, meta_out, meta_in, ghost_out, ghost_in, load_sem, pair_sem, entered = refs[13:]
    dest, send, block, restriction, own, tension = held
    me = lax.axis_index("ep")
    tiles = tension.shape[0]
    quad, nodes = restriction.shape
    cap, blocks, groups, vectors = layout(n, tiles, tension.shape[1], nodes)
    rows_e = block.shape[0]
    halves = own.shape[0]
    wide = tiles * halves
    slots = n * cap
    cuts = tension.shape[1] // DEPTH

    small = [pltpu.make_async_copy(a, b, load_sem.at[i]) for i, (a, b) in enumerate(zip(given[:5], held[:5]))]
    rows = tiles // LOADS
    pieces_of = [pl.ds(c * rows, rows) for c in range(LOADS)]
    columns = [pltpu.make_async_copy(given[5].at[c], tension.at[c], load_sem.at[5]) for c in pieces_of]
    for load in small[:1] + columns + small[1:]:
        load.start()

    barrier = pltpu.get_barrier_semaphore()

    def each(first, last, step):
        lax.fori_loop(first, last, lambda p, _: (step(p), 0)[1], 0)

    each(me + 1, n, lambda p: pl.semaphore_signal(barrier, inc=1, device_id={"ep": p}))

    last = n - 1
    edges = stages(n)
    parts_of = [range(a, b) for a, b in zip((0,) + edges, edges + (n,))]
    count = len(parts_of)
    my_part = sum((me >= edge).astype(I32) for edge in edges)

    def remote(src, dst, sent, got, peer):
        return pltpu.make_async_remote_copy(
            src_ref=src, dst_ref=dst, send_sem=pair_sem.at[sent], recv_sem=pair_sem.at[got], device_id={"ep": peer}
        )

    def send_meta(p):
        remote(meta_out.at[p], meta_in.at[me], 0, 4 + my_part, p).start()

    def send_data(p):
        remote(outbox.at[p], inbox.at[me], 1, 4 + count + my_part, p).start()

    def send_both(p):
        send_meta(p)
        send_data(p)

    def several(a, b, many, sent, got):
        return remote(a.at[pl.ds(0, many)], b.at[pl.ds(0, many)], sent, got, lax.rem(me + 1, n))

    ghosts = remote(ghost_out, ghost_in, 2, 3, lax.rem(me + last, n))

    small[0].wait()
    small[3].wait()
    place = dest[...]
    target = lax.div(place, tiles)
    to_peer = (jnp.broadcast_to(target, (n, tiles)) == iota((n, tiles), 0)).astype(F32)
    earlier = onehot(iota((tiles, tiles), 0) < iota((tiles, tiles), 1))
    before = jnp.dot(to_peer.astype(BF16), earlier, preferred_element_type=F32)
    rank = jnp.sum(before * to_peer, axis=0, keepdims=True).astype(I32)
    at_rank = onehot(jnp.broadcast_to(rank, (tiles, tiles)) == lax.rem(iota((tiles, tiles), 0), cap))
    position = (lax.rem(place, tiles) + 1).astype(F32)
    wanted = jnp.concatenate([to_peer * iota((n, tiles), 1).astype(F32), to_peer * position], axis=0)
    wanted = minor_dot(wanted.astype(BF16), at_rank)
    tile_of, where_to = wanted[:n].astype(I32), wanted[n:]
    for p in range(n):
        meta_out[p, 0:1, :] = where_to[p : p + 1]
        meta_out[(p + n - 1) % n, 1:2, :] = where_to[p : p + 1]

    full = (DEPTH // nodes * quad, DEPTH)
    weight = jnp.concatenate([restriction[...]] * (DEPTH // nodes), axis=1)
    weight = jnp.concatenate([weight] * (DEPTH // nodes), axis=0)
    weight = jnp.where(lax.div(iota(full, 0), quad) == lax.div(iota(full, 1), nodes), weight, 0.0)
    weight = jnp.concatenate(pieces(weight), axis=0)

    @pl.when(me > 0)
    def _():
        pl.semaphore_wait(barrier, me)
        send_meta(0)

    pltpu.make_async_copy(given[5], tension, load_sem.at[5]).wait()
    local = []
    for c in range(cuts):
        both = jnp.concatenate(pieces(tension[:, c * DEPTH : (c + 1) * DEPTH]), axis=0)
        part = minor_dot(weight, both)
        local.append(part[: full[0], :tiles] + (part[: full[0], tiles:] + part[full[0] :, :tiles]))
    local = jnp.concatenate(local, axis=0)
    group = lax.div(iota((quad, tiles), 1), cap)

    def pack(p):
        index = jnp.broadcast_to(tile_of[p : p + 1], (quad, tiles))
        for v in range(vectors):
            low = v * groups * quad
            got = lanes_of(local[low : low + quad], index)
            for g in range(1, groups):
                low = (v * groups + g) * quad
                got = jnp.where(group == g, lanes_of(local[low : low + quad], index), got)
            outbox[p, v * quad : (v + 1) * quad, :] = got
            outbox[(p + n - 1) % n, (vectors + v) * quad : (vectors + v + 1) * quad, :] = got

    pack(0)
    pack(1)

    each(0, jnp.minimum(me, 1), send_data)
    each(0, me, lambda p: pl.semaphore_signal(entered.at[me], inc=1, device_id={"ep": p}))
    small[1].wait()
    small[2].wait()
    for h in range(halves):
        want = jnp.broadcast_to(send[h : h + 1, :], (rows_e, tiles))
        got = lanes_of(block[...], lax.rem(want, tiles))
        ghost_out[h : h + 1, :] = jnp.sum(
            jnp.where(lax.div(want, tiles) == iota((rows_e, tiles), 0), got, 0), axis=0, keepdims=True
        )

    @pl.when(me > 0)
    def _():
        ghosts.start()

    for p in range(2, n):
        pack(p)
    each(1, me, send_both)

    def up(p):
        pl.semaphore_wait(entered.at[p], 1)
        send_both(p)

    each(me + 1, n, up)

    @pl.when(me == 0)
    def _():
        ghosts.start()

    meta_in[me] = meta_out[me]
    inbox[me] = outbox[me]

    small[4].wait()
    owned = jnp.concatenate([own[h : h + 1, :] for h in range(halves)], axis=1)
    entry = (iota((rows_e, wide), 1) + 1).astype(F32)
    entry = jnp.where(
        jnp.broadcast_to(lax.div(owned, tiles), (rows_e, wide)) == iota((rows_e, wide), 0), entry, 0.0
    ).astype(BF16)
    column = jnp.broadcast_to(lax.rem(owned, tiles), (tiles, wide)) == iota((tiles, wide), 0)
    shared = minor_dot(entry, onehot(column)).astype(I32)

    which = jnp.maximum(shared - 1, 0)
    ghosts.wait_recv()
    other = jnp.zeros((rows_e, tiles), I32)
    for h in range(halves):
        row = jnp.broadcast_to(ghost_in[h : h + 1, :], (rows_e, tiles))
        other = jnp.where(lax.div(which, tiles) == h, lanes_of(row, lax.rem(which, tiles)), other)

    per = tiles // cap
    lane = lax.div(iota((1, tiles), 1), cap)

    def came_in(sources):
        first = sources[0] // per
        spans = range(first, sources[-1] // per + 1)
        hits = []
        for kind in range(2):
            parts = []
            for h in spans:
                pos = jnp.zeros((1, tiles), F32)
                for s in range(per):
                    if h * per + s in sources:
                        pos = jnp.where(lane == s, meta_in[h * per + s, kind : kind + 1, :], pos)
                pos = jnp.broadcast_to(pos.astype(I32), (tiles, tiles))
                parts.append(onehot(pos == iota((tiles, tiles), 0) + 1))
            hits.append(jnp.concatenate(parts, axis=1))
        number = iota((rows_e, len(spans) * tiles), 1) + (first * tiles + 1)
        return minor_dot(number.astype(F32).astype(BF16), jnp.concatenate(hits, axis=0)).astype(I32)

    def find(index, table):
        slot = lanes_of(table, lax.div(index, blocks))
        part = lax.rem(index, blocks)
        there = jnp.maximum(slot - 1, 0)
        vector = lax.div(there, cap) * vectors + lax.div(part, groups)
        return lax.rem(part, groups) * cap + lax.rem(there, cap), jnp.where(slot > 0, vector, -1)

    def find_all(sources):
        table = came_in(sources)
        return find(block[...], table[:, :tiles]) + find(other, table[:, tiles:])

    def spread(x, r):
        return jnp.broadcast_to(x[r : r + 1, :], (quad, tiles))

    def take(r, lane_at, vector_at, base, first, end, got):
        index, vector = spread(lane_at, r), spread(vector_at, r)

        def step(s, got):
            for v in range(vectors):
                low = base + v * quad
                here = lanes_of(inbox[s, low : low + quad, :], index)
                got = jnp.where(vector == s * vectors + v, here, got)
            return got

        return lax.fori_loop(first, end, step, got, unroll=end - first <= 16)

    def take_all(found, first, end, mine, theirs):
        for r in range(rows_e):
            mine[r] = take(r, found[0], found[1], 0, first, end, mine[r])
            theirs[r] = take(r, found[2], found[3], vectors * quad, first, end, theirs[r])

    def arrived(a, b, sent, got, sources):
        ours = (me >= sources[0]) & (me <= sources[-1])
        for many, there in ((len(sources) - 1, ours), (len(sources), jnp.logical_not(ours))):
            if many:

                @pl.when(there)
                def _():
                    several(a, b, many, sent, got).wait_recv()

    mine = [jnp.zeros((quad, tiles), F32)] * rows_e
    theirs = [jnp.zeros((quad, tiles), F32)] * rows_e
    arrived(meta_out, meta_in, 0, 4, parts_of[0])
    found = find_all(parts_of[0])
    for i, sources in enumerate(parts_of):
        arrived(outbox, inbox, 1, 4 + count + i, sources)
        if i + 1 < count:
            arrived(meta_out, meta_in, 0, 5 + i, parts_of[i + 1])
        take_all(found, sources[0], sources[-1] + 1, mine, theirs)
        if i + 1 < count:
            found = find_all(parts_of[i + 1])
    for r in range(rows_e):
        out[:, r * tiles : (r + 1) * tiles] = jnp.where(
            spread(shared, r) > 0, 0.5 * (mine[r] + theirs[r]), mine[r]
        )

    ghosts.wait_send()
    several(meta_out, meta_in, last, 0, 4).wait_send()
    several(outbox, inbox, last, 1, 4 + count).wait_send()


def per_device(tension, tile_dest, restriction, elem_block, shared_own, shared_send):
    n = lax.axis_size("ep")
    tiles = tension.shape[0]
    quad, nodes = restriction.shape
    vectors = layout(n, tiles, tension.shape[1], nodes)[3]
    halves = shared_own.shape[0] // tiles
    given = (
        tile_dest.reshape(1, tiles),
        shared_send.reshape(halves, tiles),
        elem_block.reshape(-1, tiles),
        restriction,
        shared_own.reshape(halves, tiles),
        tension,
    )
    return pl.pallas_call(
        functools.partial(kernel, n),
        out_shape=jax.ShapeDtypeStruct((quad, elem_block.shape[0]), F32),
        in_specs=[pl.BlockSpec(memory_space=pltpu.HBM)] * 6,
        out_specs=pl.BlockSpec(memory_space=pltpu.VMEM),
        scratch_shapes=[pltpu.VMEM(a.shape, a.dtype) for a in given]
        + [
            pltpu.VMEM((n, 2 * vectors * quad, tiles), F32),
            pltpu.VMEM((n, 2 * vectors * quad, tiles), F32),
            pltpu.VMEM((n, 2, tiles), F32),
            pltpu.VMEM((n, 2, tiles), F32),
            pltpu.VMEM((halves, tiles), I32),
            pltpu.VMEM((halves, tiles), I32),
            pltpu.SemaphoreType.DMA((6,)),
            pltpu.SemaphoreType.DMA((4 + 2 * (len(stages(n)) + 1),)),
            pltpu.SemaphoreType.REGULAR((n,)),
        ],
        compiler_params=pltpu.CompilerParams(
            collective_id=0, has_side_effects=True, vmem_limit_bytes=16 * 2**20
        ),
    )(*[pltpu.with_memory_space_constraint(a, pltpu.HBM) for a in given])


def solution(mesh):
    return jax.shard_map(
        per_device,
        mesh=mesh,
        in_specs=(
            P(("rep", "ep"), None),
            P(("rep", "ep")),
            P(),
            P(("rep", "ep")),
            P(("rep", "ep")),
            P(("rep", "ep")),
        ),
        out_specs=P(None, ("rep", "ep")),
        check_vma=False,
    )
```

```python
import functools

import jax
import jax.numpy as jnp
from jax import lax
from jax.experimental import pallas as pl
from jax.experimental.pallas import tpu as pltpu
from jax.sharding import PartitionSpec as P

F32 = jnp.float32
BF16 = jnp.bfloat16
I32 = jnp.int32
MINOR = (((1,), (1,)), ((), ()))
DEPTH = 256
LOADS = 8
HOLD = 1800


def iota(shape, dim):
    return lax.broadcasted_iota(I32, shape, dim)


def pieces(x):
    high = x.astype(BF16)
    return high, (x - high.astype(F32)).astype(BF16)


def onehot(x):
    return x.astype(F32).astype(BF16)


def minor_dot(a, b):
    return lax.dot_general(a, b, MINOR, preferred_element_type=F32)


def lanes_of(x, index):
    return jnp.take_along_axis(x, index, axis=1, mode="promise_in_bounds")


def layout(n, tiles, nodal, nodes):
    cap = 2 * tiles // n
    blocks = nodal // nodes
    groups = min(tiles // cap, blocks)
    return cap, blocks, groups, blocks // groups


def stages(n):
    return (n // 2 + 1, n - 1)


def kernel(n, *refs):
    given, out, held = refs[:6], refs[6], refs[7:13]
    outbox, inbox, meta_out, meta_in, ghost_out, ghost_in, load_sem, pair_sem, entered = refs[13:]
    dest, send, block, restriction, own, tension = held
    me = lax.axis_index("ep")
    tiles = tension.shape[0]
    quad, nodes = restriction.shape
    cap, blocks, groups, vectors = layout(n, tiles, tension.shape[1], nodes)
    rows_e = block.shape[0]
    halves = own.shape[0]
    wide = tiles * halves
    slots = n * cap
    cuts = tension.shape[1] // DEPTH

    small = [pltpu.make_async_copy(a, b, load_sem.at[i]) for i, (a, b) in enumerate(zip(given[:5], held[:5]))]
    rows = tiles // LOADS
    pieces_of = [pl.ds(c * rows, rows) for c in range(LOADS)]
    columns = [pltpu.make_async_copy(given[5].at[c], tension.at[c], load_sem.at[5]) for c in pieces_of]
    for load in small[:1] + columns + small[1:]:
        load.start()

    barrier = pltpu.get_barrier_semaphore()

    def each(first, last, step):
        lax.fori_loop(first, last, lambda p, _: (step(p), 0)[1], 0)

    each(me + 1, n, lambda p: pl.semaphore_signal(barrier, inc=1, device_id={"ep": p}))

    last = n - 1
    edges = stages(n)
    parts_of = [range(a, b) for a, b in zip((0,) + edges, edges + (n,))]
    count = len(parts_of)
    my_part = sum((me >= edge).astype(I32) for edge in edges)

    def remote(src, dst, sent, got, peer):
        return pltpu.make_async_remote_copy(
            src_ref=src, dst_ref=dst, send_sem=pair_sem.at[sent], recv_sem=pair_sem.at[got], device_id={"ep": peer}
        )

    def send_meta(p):
        remote(meta_out.at[p], meta_in.at[me], 0, 4 + my_part, p).start()

    def send_data(p):
        remote(outbox.at[p], inbox.at[me], 1, 4 + count + my_part, p).start()

    def send_both(p):
        send_meta(p)
        send_data(p)

    def several(a, b, many, sent, got):
        return remote(a.at[pl.ds(0, many)], b.at[pl.ds(0, many)], sent, got, lax.rem(me + 1, n))

    ghosts = remote(ghost_out, ghost_in, 2, 3, lax.rem(me + last, n))

    small[0].wait()
    small[3].wait()
    place = dest[...]
    target = lax.div(place, tiles)
    to_peer = (jnp.broadcast_to(target, (n, tiles)) == iota((n, tiles), 0)).astype(F32)
    earlier = onehot(iota((tiles, tiles), 0) < iota((tiles, tiles), 1))
    before = jnp.dot(to_peer.astype(BF16), earlier, preferred_element_type=F32)
    rank = jnp.sum(before * to_peer, axis=0, keepdims=True).astype(I32)
    at_rank = onehot(jnp.broadcast_to(rank, (tiles, tiles)) == lax.rem(iota((tiles, tiles), 0), cap))
    position = (lax.rem(place, tiles) + 1).astype(F32)
    wanted = jnp.concatenate([to_peer * iota((n, tiles), 1).astype(F32), to_peer * position], axis=0)
    wanted = minor_dot(wanted.astype(BF16), at_rank)
    tile_of, where_to = wanted[:n].astype(I32), wanted[n:]
    for p in range(n):
        meta_out[p, 0:1, :] = where_to[p : p + 1]
        meta_out[(p + n - 1) % n, 1:2, :] = where_to[p : p + 1]

    full = (DEPTH // nodes * quad, DEPTH)
    weight = jnp.concatenate([restriction[...]] * (DEPTH // nodes), axis=1)
    weight = jnp.concatenate([weight] * (DEPTH // nodes), axis=0)
    weight = jnp.where(lax.div(iota(full, 0), quad) == lax.div(iota(full, 1), nodes), weight, 0.0)
    weight = jnp.concatenate(pieces(weight), axis=0)

    @pl.when(me > 0)
    def _():
        pl.semaphore_wait(barrier, me)
        send_meta(0)

    pltpu.make_async_copy(given[5], tension, load_sem.at[5]).wait()
    local = []
    for c in range(cuts):
        both = jnp.concatenate(pieces(tension[:, c * DEPTH : (c + 1) * DEPTH]), axis=0)
        part = minor_dot(weight, both)
        local.append(part[: full[0], :tiles] + (part[: full[0], tiles:] + part[full[0] :, :tiles]))
    local = jnp.concatenate(local, axis=0)
    group = lax.div(iota((quad, tiles), 1), cap)

    def pack(p):
        index = jnp.broadcast_to(tile_of[p : p + 1], (quad, tiles))
        for v in range(vectors):
            low = v * groups * quad
            got = lanes_of(local[low : low + quad], index)
            for g in range(1, groups):
                low = (v * groups + g) * quad
                got = jnp.where(group == g, lanes_of(local[low : low + quad], index), got)
            outbox[p, v * quad : (v + 1) * quad, :] = got
            outbox[(p + n - 1) % n, (vectors + v) * quad : (vectors + v + 1) * quad, :] = got

    pack(0)
    pack(1)

    each(0, jnp.minimum(me, 1), send_data)
    each(0, me, lambda p: pl.semaphore_signal(entered.at[me], inc=1, device_id={"ep": p}))
    small[1].wait()
    small[2].wait()
    for h in range(halves):
        want = jnp.broadcast_to(send[h : h + 1, :], (rows_e, tiles))
        got = lanes_of(block[...], lax.rem(want, tiles))
        ghost_out[h : h + 1, :] = jnp.sum(
            jnp.where(lax.div(want, tiles) == iota((rows_e, tiles), 0), got, 0), axis=0, keepdims=True
        )

    @pl.when(me > 0)
    def _():
        ghosts.start()

    for p in range(2, n):
        pack(p)

    @pl.when(lax.rem(lax.axis_index("rep"), 2) == 1)
    def _():
        pl.delay(HOLD)

    each(1, me, send_both)

    def up(p):
        pl.semaphore_wait(entered.at[p], 1)
        send_both(p)

    each(me + 1, n, up)

    @pl.when(me == 0)
    def _():
        ghosts.start()

    meta_in[me] = meta_out[me]
    inbox[me] = outbox[me]

    small[4].wait()
    owned = jnp.concatenate([own[h : h + 1, :] for h in range(halves)], axis=1)
    entry = (iota((rows_e, wide), 1) + 1).astype(F32)
    entry = jnp.where(
        jnp.broadcast_to(lax.div(owned, tiles), (rows_e, wide)) == iota((rows_e, wide), 0), entry, 0.0
    ).astype(BF16)
    column = jnp.broadcast_to(lax.rem(owned, tiles), (tiles, wide)) == iota((tiles, wide), 0)
    shared = minor_dot(entry, onehot(column)).astype(I32)

    which = jnp.maximum(shared - 1, 0)
    ghosts.wait_recv()
    other = jnp.zeros((rows_e, tiles), I32)
    for h in range(halves):
        row = jnp.broadcast_to(ghost_in[h : h + 1, :], (rows_e, tiles))
        other = jnp.where(lax.div(which, tiles) == h, lanes_of(row, lax.rem(which, tiles)), other)

    per = tiles // cap
    lane = lax.div(iota((1, tiles), 1), cap)

    def came_in(sources):
        first = sources[0] // per
        spans = range(first, sources[-1] // per + 1)
        hits = []
        for kind in range(2):
            parts = []
            for h in spans:
                pos = jnp.zeros((1, tiles), F32)
                for s in range(per):
                    if h * per + s in sources:
                        pos = jnp.where(lane == s, meta_in[h * per + s, kind : kind + 1, :], pos)
                pos = jnp.broadcast_to(pos.astype(I32), (tiles, tiles))
                parts.append(onehot(pos == iota((tiles, tiles), 0) + 1))
            hits.append(jnp.concatenate(parts, axis=1))
        number = iota((rows_e, len(spans) * tiles), 1) + (first * tiles + 1)
        return minor_dot(number.astype(F32).astype(BF16), jnp.concatenate(hits, axis=0)).astype(I32)

    def find(index, table):
        slot = lanes_of(table, lax.div(index, blocks))
        part = lax.rem(index, blocks)
        there = jnp.maximum(slot - 1, 0)
        vector = lax.div(there, cap) * vectors + lax.div(part, groups)
        return lax.rem(part, groups) * cap + lax.rem(there, cap), jnp.where(slot > 0, vector, -1)

    def find_all(sources):
        table = came_in(sources)
        return find(block[...], table[:, :tiles]) + find(other, table[:, tiles:])

    def spread(x, r):
        return jnp.broadcast_to(x[r : r + 1, :], (quad, tiles))

    def take(r, lane_at, vector_at, base, first, end, got):
        index, vector = spread(lane_at, r), spread(vector_at, r)

        def step(s, got):
            for v in range(vectors):
                low = base + v * quad
                here = lanes_of(inbox[s, low : low + quad, :], index)
                got = jnp.where(vector == s * vectors + v, here, got)
            return got

        return lax.fori_loop(first, end, step, got, unroll=end - first <= 16)

    def take_all(found, first, end, mine, theirs):
        for r in range(rows_e):
            mine[r] = take(r, found[0], found[1], 0, first, end, mine[r])
            theirs[r] = take(r, found[2], found[3], vectors * quad, first, end, theirs[r])

    def arrived(a, b, sent, got, sources):
        ours = (me >= sources[0]) & (me <= sources[-1])
        for many, there in ((len(sources) - 1, ours), (len(sources), jnp.logical_not(ours))):
            if many:

                @pl.when(there)
                def _():
                    several(a, b, many, sent, got).wait_recv()

    mine = [jnp.zeros((quad, tiles), F32)] * rows_e
    theirs = [jnp.zeros((quad, tiles), F32)] * rows_e
    arrived(meta_out, meta_in, 0, 4, parts_of[0])
    found = find_all(parts_of[0])
    for i, sources in enumerate(parts_of):
        arrived(outbox, inbox, 1, 4 + count + i, sources)
        if i + 1 < count:
            arrived(meta_out, meta_in, 0, 5 + i, parts_of[i + 1])
        take_all(found, sources[0], sources[-1] + 1, mine, theirs)
        if i + 1 < count:
            found = find_all(parts_of[i + 1])
    for r in range(rows_e):
        out[:, r * tiles : (r + 1) * tiles] = jnp.where(
            spread(shared, r) > 0, 0.5 * (mine[r] + theirs[r]), mine[r]
        )

    ghosts.wait_send()
    several(meta_out, meta_in, last, 0, 4).wait_send()
    several(outbox, inbox, last, 1, 4 + count).wait_send()


def per_device(tension, tile_dest, restriction, elem_block, shared_own, shared_send):
    n = lax.axis_size("ep")
    tiles = tension.shape[0]
    quad, nodes = restriction.shape
    vectors = layout(n, tiles, tension.shape[1], nodes)[3]
    halves = shared_own.shape[0] // tiles
    given = (
        tile_dest.reshape(1, tiles),
        shared_send.reshape(halves, tiles),
        elem_block.reshape(-1, tiles),
        restriction,
        shared_own.reshape(halves, tiles),
        tension,
    )
    return pl.pallas_call(
        functools.partial(kernel, n),
        out_shape=jax.ShapeDtypeStruct((quad, elem_block.shape[0]), F32),
        in_specs=[pl.BlockSpec(memory_space=pltpu.HBM)] * 6,
        out_specs=pl.BlockSpec(memory_space=pltpu.VMEM),
        scratch_shapes=[pltpu.VMEM(a.shape, a.dtype) for a in given]
        + [
            pltpu.VMEM((n, 2 * vectors * quad, tiles), F32),
            pltpu.VMEM((n, 2 * vectors * quad, tiles), F32),
            pltpu.VMEM((n, 2, tiles), F32),
            pltpu.VMEM((n, 2, tiles), F32),
            pltpu.VMEM((halves, tiles), I32),
            pltpu.VMEM((halves, tiles), I32),
            pltpu.SemaphoreType.DMA((6,)),
            pltpu.SemaphoreType.DMA((4 + 2 * (len(stages(n)) + 1),)),
            pltpu.SemaphoreType.REGULAR((n,)),
        ],
        compiler_params=pltpu.CompilerParams(
            collective_id=0, has_side_effects=True, vmem_limit_bytes=16 * 2**20
        ),
    )(*[pltpu.with_memory_space_constraint(a, pltpu.HBM) for a in given])


def solution(mesh):
    return jax.shard_map(
        per_device,
        mesh=mesh,
        in_specs=(
            P(("rep", "ep"), None),
            P(("rep", "ep")),
            P(),
            P(("rep", "ep")),
            P(("rep", "ep")),
            P(("rep", "ep")),
        ),
        out_specs=P(None, ("rep", "ep")),
        check_vma=False,
    )
```

```python
import functools

import jax
import jax.numpy as jnp
from jax import lax
from jax.experimental import pallas as pl
from jax.experimental.pallas import tpu as pltpu
from jax.sharding import PartitionSpec as P

F32 = jnp.float32
BF16 = jnp.bfloat16
I32 = jnp.int32
MINOR = (((1,), (1,)), ((), ()))
DEPTH = 256
LOADS = 8
HOLD = 1500


def iota(shape, dim):
    return lax.broadcasted_iota(I32, shape, dim)


def pieces(x):
    high = x.astype(BF16)
    return high, (x - high.astype(F32)).astype(BF16)


def onehot(x):
    return x.astype(F32).astype(BF16)


def minor_dot(a, b):
    return lax.dot_general(a, b, MINOR, preferred_element_type=F32)


def lanes_of(x, index):
    return jnp.take_along_axis(x, index, axis=1, mode="promise_in_bounds")


def layout(n, tiles, nodal, nodes):
    cap = 2 * tiles // n
    blocks = nodal // nodes
    groups = min(tiles // cap, blocks)
    return cap, blocks, groups, blocks // groups


def stages(n):
    return (n // 2 + 1, n - 1)


def kernel(n, *refs):
    given, out, held = refs[:6], refs[6], refs[7:13]
    outbox, inbox, meta_out, meta_in, ghost_out, ghost_in, load_sem, pair_sem, entered = refs[13:]
    dest, send, block, restriction, own, tension = held
    me = lax.axis_index("ep")
    tiles = tension.shape[0]
    quad, nodes = restriction.shape
    cap, blocks, groups, vectors = layout(n, tiles, tension.shape[1], nodes)
    rows_e = block.shape[0]
    halves = own.shape[0]
    wide = tiles * halves
    slots = n * cap
    cuts = tension.shape[1] // DEPTH

    small = [pltpu.make_async_copy(a, b, load_sem.at[i]) for i, (a, b) in enumerate(zip(given[:5], held[:5]))]
    rows = tiles // LOADS
    pieces_of = [pl.ds(c * rows, rows) for c in range(LOADS)]
    columns = [pltpu.make_async_copy(given[5].at[c], tension.at[c], load_sem.at[5]) for c in pieces_of]
    for load in small[:1] + columns + small[1:]:
        load.start()

    barrier = pltpu.get_barrier_semaphore()

    def each(first, last, step):
        lax.fori_loop(first, last, lambda p, _: (step(p), 0)[1], 0)

    each(me + 1, n, lambda p: pl.semaphore_signal(barrier, inc=1, device_id={"ep": p}))

    last = n - 1
    edges = stages(n)
    parts_of = [range(a, b) for a, b in zip((0,) + edges, edges + (n,))]
    count = len(parts_of)
    my_part = sum((me >= edge).astype(I32) for edge in edges)

    def remote(src, dst, sent, got, peer):
        return pltpu.make_async_remote_copy(
            src_ref=src, dst_ref=dst, send_sem=pair_sem.at[sent], recv_sem=pair_sem.at[got], device_id={"ep": peer}
        )

    def send_meta(p):
        remote(meta_out.at[p], meta_in.at[me], 0, 4 + my_part, p).start()

    def send_data(p):
        remote(outbox.at[p], inbox.at[me], 1, 4 + count + my_part, p).start()

    def send_both(p):
        send_meta(p)
        send_data(p)

    def several(a, b, many, sent, got):
        return remote(a.at[pl.ds(0, many)], b.at[pl.ds(0, many)], sent, got, lax.rem(me + 1, n))

    ghosts = remote(ghost_out, ghost_in, 2, 3, lax.rem(me + last, n))

    small[0].wait()
    small[3].wait()
    place = dest[...]
    target = lax.div(place, tiles)
    to_peer = (jnp.broadcast_to(target, (n, tiles)) == iota((n, tiles), 0)).astype(F32)
    earlier = onehot(iota((tiles, tiles), 0) < iota((tiles, tiles), 1))
    before = jnp.dot(to_peer.astype(BF16), earlier, preferred_element_type=F32)
    rank = jnp.sum(before * to_peer, axis=0, keepdims=True).astype(I32)
    at_rank = onehot(jnp.broadcast_to(rank, (tiles, tiles)) == lax.rem(iota((tiles, tiles), 0), cap))
    position = (lax.rem(place, tiles) + 1).astype(F32)
    wanted = jnp.concatenate([to_peer * iota((n, tiles), 1).astype(F32), to_peer * position], axis=0)
    wanted = minor_dot(wanted.astype(BF16), at_rank)
    tile_of, where_to = wanted[:n].astype(I32), wanted[n:]
    for p in range(n):
        meta_out[p, 0:1, :] = where_to[p : p + 1]
        meta_out[(p + n - 1) % n, 1:2, :] = where_to[p : p + 1]

    full = (DEPTH // nodes * quad, DEPTH)
    weight = jnp.concatenate([restriction[...]] * (DEPTH // nodes), axis=1)
    weight = jnp.concatenate([weight] * (DEPTH // nodes), axis=0)
    weight = jnp.where(lax.div(iota(full, 0), quad) == lax.div(iota(full, 1), nodes), weight, 0.0)
    weight = jnp.concatenate(pieces(weight), axis=0)

    @pl.when(me > 0)
    def _():
        pl.semaphore_wait(barrier, me)
        send_meta(0)

    pltpu.make_async_copy(given[5], tension, load_sem.at[5]).wait()
    local = []
    for c in range(cuts):
        both = jnp.concatenate(pieces(tension[:, c * DEPTH : (c + 1) * DEPTH]), axis=0)
        part = minor_dot(weight, both)
        local.append(part[: full[0], :tiles] + (part[: full[0], tiles:] + part[full[0] :, :tiles]))
    local = jnp.concatenate(local, axis=0)
    group = lax.div(iota((quad, tiles), 1), cap)

    def pack(p):
        index = jnp.broadcast_to(tile_of[p : p + 1], (quad, tiles))
        for v in range(vectors):
            low = v * groups * quad
            got = lanes_of(local[low : low + quad], index)
            for g in range(1, groups):
                low = (v * groups + g) * quad
                got = jnp.where(group == g, lanes_of(local[low : low + quad], index), got)
            outbox[p, v * quad : (v + 1) * quad, :] = got
            outbox[(p + n - 1) % n, (vectors + v) * quad : (vectors + v + 1) * quad, :] = got

    pack(0)
    pack(1)

    @pl.when(me > 0)
    def _():
        send_data(0)

    small[1].wait()
    small[2].wait()
    each(0, me, lambda p: pl.semaphore_signal(entered.at[me], inc=1, device_id={"ep": p}))
    for h in range(halves):
        want = jnp.broadcast_to(send[h : h + 1, :], (rows_e, tiles))
        got = lanes_of(block[...], lax.rem(want, tiles))
        ghost_out[h : h + 1, :] = jnp.sum(
            jnp.where(lax.div(want, tiles) == iota((rows_e, tiles), 0), got, 0), axis=0, keepdims=True
        )

    @pl.when(me > 0)
    def _():
        ghosts.start()

    for p in range(2, n):
        pack(p)

    @pl.when(lax.rem(lax.axis_index("rep"), 2) == 1)
    def _():
        pl.delay(HOLD)

    each(1, me, send_both)

    def up(p):
        pl.semaphore_wait(entered.at[p], 1)
        send_both(p)

    each(me + 1, n, up)

    @pl.when(me == 0)
    def _():
        ghosts.start()

    meta_in[me] = meta_out[me]
    inbox[me] = outbox[me]

    small[4].wait()
    owned = jnp.concatenate([own[h : h + 1, :] for h in range(halves)], axis=1)
    entry = (iota((rows_e, wide), 1) + 1).astype(F32)
    entry = jnp.where(
        jnp.broadcast_to(lax.div(owned, tiles), (rows_e, wide)) == iota((rows_e, wide), 0), entry, 0.0
    ).astype(BF16)
    column = jnp.broadcast_to(lax.rem(owned, tiles), (tiles, wide)) == iota((tiles, wide), 0)
    shared = minor_dot(entry, onehot(column)).astype(I32)

    which = jnp.maximum(shared - 1, 0)
    ghosts.wait_recv()
    other = jnp.zeros((rows_e, tiles), I32)
    for h in range(halves):
        row = jnp.broadcast_to(ghost_in[h : h + 1, :], (rows_e, tiles))
        other = jnp.where(lax.div(which, tiles) == h, lanes_of(row, lax.rem(which, tiles)), other)

    per = tiles // cap
    lane = lax.div(iota((1, tiles), 1), cap)

    def came_in(sources):
        first = sources[0] // per
        spans = range(first, sources[-1] // per + 1)
        hits = []
        for kind in range(2):
            parts = []
            for h in spans:
                pos = jnp.zeros((1, tiles), F32)
                for s in range(per):
                    if h * per + s in sources:
                        pos = jnp.where(lane == s, meta_in[h * per + s, kind : kind + 1, :], pos)
                pos = jnp.broadcast_to(pos.astype(I32), (tiles, tiles))
                parts.append(onehot(pos == iota((tiles, tiles), 0) + 1))
            hits.append(jnp.concatenate(parts, axis=1))
        number = iota((rows_e, len(spans) * tiles), 1) + (first * tiles + 1)
        return minor_dot(number.astype(F32).astype(BF16), jnp.concatenate(hits, axis=0)).astype(I32)

    def find(index, table):
        slot = lanes_of(table, lax.div(index, blocks))
        part = lax.rem(index, blocks)
        there = jnp.maximum(slot - 1, 0)
        vector = lax.div(there, cap) * vectors + lax.div(part, groups)
        return lax.rem(part, groups) * cap + lax.rem(there, cap), jnp.where(slot > 0, vector, -1)

    def find_all(sources):
        table = came_in(sources)
        return find(block[...], table[:, :tiles]) + find(other, table[:, tiles:])

    def spread(x, r):
        return jnp.broadcast_to(x[r : r + 1, :], (quad, tiles))

    def take(r, lane_at, vector_at, base, first, end, got):
        index, vector = spread(lane_at, r), spread(vector_at, r)

        def step(s, got):
            for v in range(vectors):
                low = base + v * quad
                here = lanes_of(inbox[s, low : low + quad, :], index)
                got = jnp.where(vector == s * vectors + v, here, got)
            return got

        return lax.fori_loop(first, end, step, got, unroll=end - first <= 16)

    def take_all(found, first, end, mine, theirs):
        for r in range(rows_e):
            mine[r] = take(r, found[0], found[1], 0, first, end, mine[r])
            theirs[r] = take(r, found[2], found[3], vectors * quad, first, end, theirs[r])

    def arrived(a, b, sent, got, sources):
        ours = (me >= sources[0]) & (me <= sources[-1])
        for many, there in ((len(sources) - 1, ours), (len(sources), jnp.logical_not(ours))):
            if many:

                @pl.when(there)
                def _():
                    several(a, b, many, sent, got).wait_recv()

    mine = [jnp.zeros((quad, tiles), F32)] * rows_e
    theirs = [jnp.zeros((quad, tiles), F32)] * rows_e
    arrived(meta_out, meta_in, 0, 4, parts_of[0])
    found = find_all(parts_of[0])
    for i, sources in enumerate(parts_of):
        arrived(outbox, inbox, 1, 4 + count + i, sources)
        if i + 1 < count:
            arrived(meta_out, meta_in, 0, 5 + i, parts_of[i + 1])
        take_all(found, sources[0], sources[-1] + 1, mine, theirs)
        if i + 1 < count:
            found = find_all(parts_of[i + 1])
    for r in range(rows_e):
        out[:, r * tiles : (r + 1) * tiles] = jnp.where(
            spread(shared, r) > 0, 0.5 * (mine[r] + theirs[r]), mine[r]
        )

    ghosts.wait_send()
    several(meta_out, meta_in, last, 0, 4).wait_send()
    several(outbox, inbox, last, 1, 4 + count).wait_send()


def per_device(tension, tile_dest, restriction, elem_block, shared_own, shared_send):
    n = lax.axis_size("ep")
    tiles = tension.shape[0]
    quad, nodes = restriction.shape
    vectors = layout(n, tiles, tension.shape[1], nodes)[3]
    halves = shared_own.shape[0] // tiles
    given = (
        tile_dest.reshape(1, tiles),
        shared_send.reshape(halves, tiles),
        elem_block.reshape(-1, tiles),
        restriction,
        shared_own.reshape(halves, tiles),
        tension,
    )
    return pl.pallas_call(
        functools.partial(kernel, n),
        out_shape=jax.ShapeDtypeStruct((quad, elem_block.shape[0]), F32),
        in_specs=[pl.BlockSpec(memory_space=pltpu.HBM)] * 6,
        out_specs=pl.BlockSpec(memory_space=pltpu.VMEM),
        scratch_shapes=[pltpu.VMEM(a.shape, a.dtype) for a in given]
        + [
            pltpu.VMEM((n, 2 * vectors * quad, tiles), F32),
            pltpu.VMEM((n, 2 * vectors * quad, tiles), F32),
            pltpu.VMEM((n, 2, tiles), F32),
            pltpu.VMEM((n, 2, tiles), F32),
            pltpu.VMEM((halves, tiles), I32),
            pltpu.VMEM((halves, tiles), I32),
            pltpu.SemaphoreType.DMA((6,)),
            pltpu.SemaphoreType.DMA((4 + 2 * (len(stages(n)) + 1),)),
            pltpu.SemaphoreType.REGULAR((n,)),
        ],
        compiler_params=pltpu.CompilerParams(
            collective_id=0, has_side_effects=True, vmem_limit_bytes=16 * 2**20
        ),
    )(*[pltpu.with_memory_space_constraint(a, pltpu.HBM) for a in given])


def solution(mesh):
    return jax.shard_map(
        per_device,
        mesh=mesh,
        in_specs=(
            P(("rep", "ep"), None),
            P(("rep", "ep")),
            P(),
            P(("rep", "ep")),
            P(("rep", "ep")),
            P(("rep", "ep")),
        ),
        out_specs=P(None, ("rep", "ep")),
        check_vma=False,
    )
```

```python
import functools

import jax
import jax.numpy as jnp
from jax import lax
from jax.experimental import pallas as pl
from jax.experimental.pallas import tpu as pltpu
from jax.sharding import PartitionSpec as P

F32 = jnp.float32
BF16 = jnp.bfloat16
I32 = jnp.int32
MINOR = (((1,), (1,)), ((), ()))
DEPTH = 256
ALONG_LANES = lax.GatherDimensionNumbers(
    offset_dims=(),
    collapsed_slice_dims=(1,),
    start_index_map=(1,),
    operand_batching_dims=(0,),
    start_indices_batching_dims=(0,),
)
LOADS = 8
HOLD = 1500


def iota(shape, dim):
    return lax.broadcasted_iota(I32, shape, dim)


def pieces(x):
    high = x.astype(BF16)
    return high, (x - high.astype(F32)).astype(BF16)


def onehot(x):
    return x.astype(F32).astype(BF16)


def minor_dot(a, b):
    return lax.dot_general(a, b, MINOR, preferred_element_type=F32)


def lanes_of(x, index):
    return lax.gather(
        x, index[..., None], ALONG_LANES, (1, 1), mode=lax.GatherScatterMode.PROMISE_IN_BOUNDS
    )


def layout(n, tiles, nodal, nodes):
    cap = 2 * tiles // n
    blocks = nodal // nodes
    groups = min(tiles // cap, blocks)
    return cap, blocks, groups, blocks // groups


def stages(n):
    return (n // 2 + 1, n - 1)


def kernel(n, *refs):
    given, out, held = refs[:6], refs[6], refs[7:13]
    outbox, inbox, meta_out, meta_in, ghost_out, ghost_in, load_sem, pair_sem, entered = refs[13:]
    dest, send, block, restriction, own, tension = held
    me = lax.axis_index("ep")
    tiles = tension.shape[0]
    quad, nodes = restriction.shape
    cap, blocks, groups, vectors = layout(n, tiles, tension.shape[1], nodes)
    rows_e = block.shape[0]
    halves = own.shape[0]
    wide = tiles * halves
    slots = n * cap
    cuts = tension.shape[1] // DEPTH

    small = [pltpu.make_async_copy(a, b, load_sem.at[i]) for i, (a, b) in enumerate(zip(given[:5], held[:5]))]
    rows = tiles // LOADS
    pieces_of = [pl.ds(c * rows, rows) for c in range(LOADS)]
    columns = [pltpu.make_async_copy(given[5].at[c], tension.at[c], load_sem.at[5]) for c in pieces_of]
    for load in small[:1] + columns + small[1:]:
        load.start()

    barrier = pltpu.get_barrier_semaphore()

    def each(first, last, step):
        lax.fori_loop(first, last, lambda p, _: (step(p), 0)[1], 0)

    each(me + 1, n, lambda p: pl.semaphore_signal(barrier, inc=1, device_id={"ep": p}))

    last = n - 1
    edges = stages(n)
    parts_of = [range(a, b) for a, b in zip((0,) + edges, edges + (n,))]
    count = len(parts_of)
    my_part = sum((me >= edge).astype(I32) for edge in edges)

    def remote(src, dst, sent, got, peer):
        return pltpu.make_async_remote_copy(
            src_ref=src, dst_ref=dst, send_sem=pair_sem.at[sent], recv_sem=pair_sem.at[got], device_id={"ep": peer}
        )

    def send_meta(p):
        remote(meta_out.at[p], meta_in.at[me], 0, 4 + my_part, p).start()

    def send_data(p):
        remote(outbox.at[p], inbox.at[me], 1, 4 + count + my_part, p).start()

    def send_both(p):
        send_meta(p)
        send_data(p)

    def several(a, b, many, sent, got):
        return remote(a.at[pl.ds(0, many)], b.at[pl.ds(0, many)], sent, got, lax.rem(me + 1, n))

    ghosts = remote(ghost_out, ghost_in, 2, 3, lax.rem(me + last, n))

    small[0].wait()
    small[3].wait()
    place = dest[...]
    target = lax.div(place, tiles)
    to_peer = (jnp.broadcast_to(target, (n, tiles)) == iota((n, tiles), 0)).astype(F32)
    earlier = onehot(iota((tiles, tiles), 0) < iota((tiles, tiles), 1))
    before = jnp.dot(to_peer.astype(BF16), earlier, preferred_element_type=F32)
    rank = jnp.sum(before * to_peer, axis=0, keepdims=True).astype(I32)
    at_rank = onehot(jnp.broadcast_to(rank, (tiles, tiles)) == lax.rem(iota((tiles, tiles), 0), cap))
    position = (lax.rem(place, tiles) + 1).astype(F32)
    wanted = jnp.concatenate([to_peer * iota((n, tiles), 1).astype(F32), to_peer * position], axis=0)
    wanted = minor_dot(wanted.astype(BF16), at_rank)
    tile_of, where_to = wanted[:n].astype(I32), wanted[n:]
    for p in range(n):
        meta_out[p, 0:1, :] = where_to[p : p + 1]
        meta_out[(p + n - 1) % n, 1:2, :] = where_to[p : p + 1]

    full = (DEPTH // nodes * quad, DEPTH)
    weight = jnp.concatenate([restriction[...]] * (DEPTH // nodes), axis=1)
    weight = jnp.concatenate([weight] * (DEPTH // nodes), axis=0)
    weight = jnp.where(lax.div(iota(full, 0), quad) == lax.div(iota(full, 1), nodes), weight, 0.0)
    weight = jnp.concatenate(pieces(weight), axis=0)

    @pl.when(me > 0)
    def _():
        pl.semaphore_wait(barrier, me)
        send_meta(0)

    pltpu.make_async_copy(given[5], tension, load_sem.at[5]).wait()
    local = []
    for c in range(cuts):
        high, low = pieces(tension[:, c * DEPTH : (c + 1) * DEPTH])
        part = minor_dot(weight, high)
        local.append(part[: full[0]] + (part[full[0] :] + minor_dot(weight[: full[0]], low)))
    local = jnp.concatenate(local, axis=0)
    group = lax.div(iota((quad, tiles), 1), cap)

    def pack(p):
        index = jnp.broadcast_to(tile_of[p : p + 1], (quad, tiles))
        for v in range(vectors):
            low = v * groups * quad
            got = lanes_of(local[low : low + quad], index)
            for g in range(1, groups):
                low = (v * groups + g) * quad
                got = jnp.where(group == g, lanes_of(local[low : low + quad], index), got)
            outbox[p, v * quad : (v + 1) * quad, :] = got
            outbox[(p + n - 1) % n, (vectors + v) * quad : (vectors + v + 1) * quad, :] = got

    pack(0)
    pack(1)

    @pl.when(me > 0)
    def _():
        send_data(0)

    small[1].wait()
    small[2].wait()
    each(0, me, lambda p: pl.semaphore_signal(entered.at[me], inc=1, device_id={"ep": p}))
    for h in range(halves):
        want = jnp.broadcast_to(send[h : h + 1, :], (rows_e, tiles))
        got = lanes_of(block[...], lax.rem(want, tiles))
        ghost_out[h : h + 1, :] = jnp.sum(
            jnp.where(lax.div(want, tiles) == iota((rows_e, tiles), 0), got, 0), axis=0, keepdims=True
        )

    @pl.when(me > 0)
    def _():
        ghosts.start()

    for p in range(2, n):
        pack(p)

    @pl.when(lax.rem(lax.axis_index("rep"), 2) == 1)
    def _():
        pl.delay(HOLD)

    each(1, me, send_both)

    def up(p):
        pl.semaphore_wait(entered.at[p], 1)
        send_both(p)

    each(me + 1, n, up)

    @pl.when(me == 0)
    def _():
        ghosts.start()

    meta_in[me] = meta_out[me]
    inbox[me] = outbox[me]

    small[4].wait()
    owned = jnp.concatenate([own[h : h + 1, :] for h in range(halves)], axis=1)
    entry = (iota((rows_e, wide), 1) + 1).astype(F32)
    entry = jnp.where(
        jnp.broadcast_to(lax.div(owned, tiles), (rows_e, wide)) == iota((rows_e, wide), 0), entry, 0.0
    ).astype(BF16)
    column = jnp.broadcast_to(lax.rem(owned, tiles), (tiles, wide)) == iota((tiles, wide), 0)
    shared = minor_dot(entry, onehot(column)).astype(I32)

    which = jnp.maximum(shared - 1, 0)
    ghosts.wait_recv()
    other = jnp.zeros((rows_e, tiles), I32)
    for h in range(halves):
        row = jnp.broadcast_to(ghost_in[h : h + 1, :], (rows_e, tiles))
        other = jnp.where(lax.div(which, tiles) == h, lanes_of(row, lax.rem(which, tiles)), other)

    per = tiles // cap
    lane = lax.div(iota((1, tiles), 1), cap)

    def came_in(sources):
        first = sources[0] // per
        spans = range(first, sources[-1] // per + 1)
        hits = []
        for kind in range(2):
            parts = []
            for h in spans:
                pos = jnp.zeros((1, tiles), F32)
                for s in range(per):
                    if h * per + s in sources:
                        pos = jnp.where(lane == s, meta_in[h * per + s, kind : kind + 1, :], pos)
                pos = jnp.broadcast_to(pos.astype(I32), (tiles, tiles))
                parts.append(onehot(pos == iota((tiles, tiles), 0) + 1))
            hits.append(jnp.concatenate(parts, axis=1))
        number = iota((rows_e, len(spans) * tiles), 1) + (first * tiles + 1)
        return minor_dot(number.astype(F32).astype(BF16), jnp.concatenate(hits, axis=0)).astype(I32)

    def find(index, table):
        slot = lanes_of(table, lax.div(index, blocks))
        part = lax.rem(index, blocks)
        there = jnp.maximum(slot - 1, 0)
        vector = lax.div(there, cap) * vectors + lax.div(part, groups)
        return lax.rem(part, groups) * cap + lax.rem(there, cap), jnp.where(slot > 0, vector, -1)

    def find_all(sources):
        table = came_in(sources)
        return find(block[...], table[:, :tiles]) + find(other, table[:, tiles:])

    def spread(x, r):
        return jnp.broadcast_to(x[r : r + 1, :], (quad, tiles))

    def take(r, lane_at, vector_at, base, first, end, got):
        index, vector = spread(lane_at, r), spread(vector_at, r)

        def step(s, got):
            for v in range(vectors):
                low = base + v * quad
                here = lanes_of(inbox[s, low : low + quad, :], index)
                got = jnp.where(vector == s * vectors + v, here, got)
            return got

        return lax.fori_loop(first, end, step, got, unroll=end - first <= 16)

    def take_all(found, first, end, mine, theirs):
        for r in range(rows_e):
            mine[r] = take(r, found[0], found[1], 0, first, end, mine[r])
            theirs[r] = take(r, found[2], found[3], vectors * quad, first, end, theirs[r])

    def arrived(a, b, sent, got, sources):
        ours = (me >= sources[0]) & (me <= sources[-1])
        for many, there in ((len(sources) - 1, ours), (len(sources), jnp.logical_not(ours))):
            if many:

                @pl.when(there)
                def _():
                    several(a, b, many, sent, got).wait_recv()

    mine = [jnp.zeros((quad, tiles), F32)] * rows_e
    theirs = [jnp.zeros((quad, tiles), F32)] * rows_e
    arrived(meta_out, meta_in, 0, 4, parts_of[0])
    found = find_all(parts_of[0])
    for i, sources in enumerate(parts_of):
        arrived(outbox, inbox, 1, 4 + count + i, sources)
        if i + 1 < count:
            arrived(meta_out, meta_in, 0, 5 + i, parts_of[i + 1])
        take_all(found, sources[0], sources[-1] + 1, mine, theirs)
        if i + 1 < count:
            found = find_all(parts_of[i + 1])
    for r in range(rows_e):
        out[:, r * tiles : (r + 1) * tiles] = jnp.where(
            spread(shared, r) > 0, 0.5 * (mine[r] + theirs[r]), mine[r]
        )

    ghosts.wait_send()
    several(meta_out, meta_in, last, 0, 4).wait_send()
    several(outbox, inbox, last, 1, 4 + count).wait_send()


def per_device(tension, tile_dest, restriction, elem_block, shared_own, shared_send):
    n = lax.axis_size("ep")
    tiles = tension.shape[0]
    quad, nodes = restriction.shape
    vectors = layout(n, tiles, tension.shape[1], nodes)[3]
    halves = shared_own.shape[0] // tiles
    given = (
        tile_dest.reshape(1, tiles),
        shared_send.reshape(halves, tiles),
        elem_block.reshape(-1, tiles),
        restriction,
        shared_own.reshape(halves, tiles),
        tension,
    )
    return pl.pallas_call(
        functools.partial(kernel, n),
        out_shape=jax.ShapeDtypeStruct((quad, elem_block.shape[0]), F32),
        in_specs=[pl.BlockSpec(memory_space=pltpu.HBM)] * 6,
        out_specs=pl.BlockSpec(memory_space=pltpu.VMEM),
        scratch_shapes=[pltpu.VMEM(a.shape, a.dtype) for a in given]
        + [
            pltpu.VMEM((n, 2 * vectors * quad, tiles), F32),
            pltpu.VMEM((n, 2 * vectors * quad, tiles), F32),
            pltpu.VMEM((n, 2, tiles), F32),
            pltpu.VMEM((n, 2, tiles), F32),
            pltpu.VMEM((halves, tiles), I32),
            pltpu.VMEM((halves, tiles), I32),
            pltpu.SemaphoreType.DMA((6,)),
            pltpu.SemaphoreType.DMA((4 + 2 * (len(stages(n)) + 1),)),
            pltpu.SemaphoreType.REGULAR((n,)),
        ],
        compiler_params=pltpu.CompilerParams(
            collective_id=0, has_side_effects=True, vmem_limit_bytes=16 * 2**20
        ),
    )(*[pltpu.with_memory_space_constraint(a, pltpu.HBM) for a in given])


def solution(mesh):
    return jax.shard_map(
        per_device,
        mesh=mesh,
        in_specs=(
            P(("rep", "ep"), None),
            P(("rep", "ep")),
            P(),
            P(("rep", "ep")),
            P(("rep", "ep")),
            P(("rep", "ep")),
        ),
        out_specs=P(None, ("rep", "ep")),
        check_vma=False,
    )
```

```python
import functools

import jax
import jax.numpy as jnp
from jax import lax
from jax.experimental import pallas as pl
from jax.experimental.pallas import tpu as pltpu
from jax.sharding import PartitionSpec as P

F32 = jnp.float32
BF16 = jnp.bfloat16
I32 = jnp.int32
MINOR = (((1,), (1,)), ((), ()))
DEPTH = 256
ALONG_LANES = lax.GatherDimensionNumbers(
    offset_dims=(),
    collapsed_slice_dims=(1,),
    start_index_map=(1,),
    operand_batching_dims=(0,),
    start_indices_batching_dims=(0,),
)
LOADS = 8
HOLD = 1500


def iota(shape, dim):
    return lax.broadcasted_iota(I32, shape, dim)


def pieces(x):
    high = x.astype(BF16)
    return high, (x - high.astype(F32)).astype(BF16)


def onehot(x):
    return x.astype(F32).astype(BF16)


def minor_dot(a, b):
    return lax.dot_general(a, b, MINOR, preferred_element_type=F32)


def lanes_of(x, index):
    return lax.gather(
        x, index[..., None], ALONG_LANES, (1, 1), mode=lax.GatherScatterMode.PROMISE_IN_BOUNDS
    )


def layout(n, tiles, nodal, nodes):
    cap = 2 * tiles // n
    blocks = nodal // nodes
    groups = min(tiles // cap, blocks)
    return cap, blocks, groups, blocks // groups


def stages(n):
    return (n // 2 + 1, n - 1)


def kernel(n, *refs):
    given, out, held = refs[:6], refs[6], refs[7:13]
    outbox, inbox, meta_out, meta_in, ghost_out, ghost_in, load_sem, pair_sem, entered = refs[13:]
    dest, send, block, restriction, own, tension = held
    me = lax.axis_index("ep")
    tiles = tension.shape[0]
    quad, nodes = restriction.shape
    cap, blocks, groups, vectors = layout(n, tiles, tension.shape[1], nodes)
    rows_e = block.shape[0]
    halves = own.shape[0]
    wide = tiles * halves
    slots = n * cap
    cuts = tension.shape[1] // DEPTH

    small = [pltpu.make_async_copy(a, b, load_sem.at[i]) for i, (a, b) in enumerate(zip(given[:5], held[:5]))]
    rows = tiles // LOADS
    pieces_of = [pl.ds(c * rows, rows) for c in range(LOADS)]
    columns = [pltpu.make_async_copy(given[5].at[c], tension.at[c], load_sem.at[5]) for c in pieces_of]
    for load in small[:1] + small[3:4] + columns + small[1:3] + small[4:]:
        load.start()

    barrier = pltpu.get_barrier_semaphore()

    def each(first, last, step):
        lax.fori_loop(first, last, lambda p, _: (step(p), 0)[1], 0)

    each(me + 1, n, lambda p: pl.semaphore_signal(barrier, inc=1, device_id={"ep": p}))

    last = n - 1
    edges = stages(n)
    parts_of = [range(a, b) for a, b in zip((0,) + edges, edges + (n,))]
    count = len(parts_of)
    my_part = sum((me >= edge).astype(I32) for edge in edges)

    def remote(src, dst, sent, got, peer):
        return pltpu.make_async_remote_copy(
            src_ref=src, dst_ref=dst, send_sem=pair_sem.at[sent], recv_sem=pair_sem.at[got], device_id={"ep": peer}
        )

    def send_meta(p):
        remote(meta_out.at[p], meta_in.at[me], 0, 4 + my_part, p).start()

    def send_data(p):
        remote(outbox.at[p], inbox.at[me], 1, 4 + count + my_part, p).start()

    def send_both(p):
        send_meta(p)
        send_data(p)

    def several(a, b, many, sent, got):
        return remote(a.at[pl.ds(0, many)], b.at[pl.ds(0, many)], sent, got, lax.rem(me + 1, n))

    ghosts = remote(ghost_out, ghost_in, 2, 3, lax.rem(me + last, n))

    small[0].wait()
    small[3].wait()
    place = dest[...]
    target = lax.div(place, tiles)
    to_peer = (jnp.broadcast_to(target, (n, tiles)) == iota((n, tiles), 0)).astype(F32)
    earlier = onehot(iota((tiles, tiles), 0) < iota((tiles, tiles), 1))
    before = jnp.dot(to_peer.astype(BF16), earlier, preferred_element_type=F32)
    rank = jnp.sum(before * to_peer, axis=0, keepdims=True).astype(I32)
    at_rank = onehot(jnp.broadcast_to(rank, (tiles, tiles)) == lax.rem(iota((tiles, tiles), 0), cap))
    position = (lax.rem(place, tiles) + 1).astype(F32)
    wanted = jnp.concatenate([to_peer * iota((n, tiles), 1).astype(F32), to_peer * position], axis=0)
    wanted = minor_dot(wanted.astype(BF16), at_rank)
    tile_of, where_to = wanted[:n].astype(I32), wanted[n:]
    for p in range(n):
        meta_out[p, 0:1, :] = where_to[p : p + 1]
        meta_out[(p + n - 1) % n, 1:2, :] = where_to[p : p + 1]

    full = (DEPTH // nodes * quad, DEPTH)
    weight = jnp.concatenate([restriction[...]] * (DEPTH // nodes), axis=1)
    weight = jnp.concatenate([weight] * (DEPTH // nodes), axis=0)
    weight = jnp.where(lax.div(iota(full, 0), quad) == lax.div(iota(full, 1), nodes), weight, 0.0)
    weight = jnp.concatenate(pieces(weight), axis=0)

    @pl.when(me > 0)
    def _():
        pl.semaphore_wait(barrier, me)
        send_meta(0)

    pltpu.make_async_copy(given[5], tension, load_sem.at[5]).wait()
    local = []
    for c in range(cuts):
        high, low = pieces(tension[:, c * DEPTH : (c + 1) * DEPTH])
        part = minor_dot(weight, high)
        local.append(part[: full[0]] + (part[full[0] :] + minor_dot(weight[: full[0]], low)))
    local = jnp.concatenate(local, axis=0)
    group = lax.div(iota((quad, tiles), 1), cap)

    def pack(p):
        index = jnp.broadcast_to(tile_of[p : p + 1], (quad, tiles))
        for v in range(vectors):
            low = v * groups * quad
            got = lanes_of(local[low : low + quad], index)
            for g in range(1, groups):
                low = (v * groups + g) * quad
                got = jnp.where(group == g, lanes_of(local[low : low + quad], index), got)
            outbox[p, v * quad : (v + 1) * quad, :] = got
            outbox[(p + n - 1) % n, (vectors + v) * quad : (vectors + v + 1) * quad, :] = got

    pack(0)
    pack(1)

    @pl.when(me > 0)
    def _():
        send_data(0)

    small[1].wait()
    small[2].wait()
    each(0, me, lambda p: pl.semaphore_signal(entered.at[me], inc=1, device_id={"ep": p}))
    for h in range(halves):
        want = jnp.broadcast_to(send[h : h + 1, :], (rows_e, tiles))
        got = lanes_of(block[...], lax.rem(want, tiles))
        ghost_out[h : h + 1, :] = jnp.sum(
            jnp.where(lax.div(want, tiles) == iota((rows_e, tiles), 0), got, 0), axis=0, keepdims=True
        )

    @pl.when(me > 0)
    def _():
        ghosts.start()

    for p in range(2, n):
        pack(p)

    @pl.when(lax.rem(lax.axis_index("rep"), 2) == 1)
    def _():
        pl.delay(HOLD)

    each(1, me, send_both)

    def up(p):
        pl.semaphore_wait(entered.at[p], 1)
        send_both(p)

    each(me + 1, n, up)

    @pl.when(me == 0)
    def _():
        ghosts.start()

    meta_in[me] = meta_out[me]
    inbox[me] = outbox[me]

    small[4].wait()
    owned = jnp.concatenate([own[h : h + 1, :] for h in range(halves)], axis=1)
    entry = (iota((rows_e, wide), 1) + 1).astype(F32)
    entry = jnp.where(
        jnp.broadcast_to(lax.div(owned, tiles), (rows_e, wide)) == iota((rows_e, wide), 0), entry, 0.0
    ).astype(BF16)
    column = jnp.broadcast_to(lax.rem(owned, tiles), (tiles, wide)) == iota((tiles, wide), 0)
    shared = minor_dot(entry, onehot(column)).astype(I32)

    which = jnp.maximum(shared - 1, 0)
    ghosts.wait_recv()
    other = jnp.zeros((rows_e, tiles), I32)
    for h in range(halves):
        row = jnp.broadcast_to(ghost_in[h : h + 1, :], (rows_e, tiles))
        other = jnp.where(lax.div(which, tiles) == h, lanes_of(row, lax.rem(which, tiles)), other)

    per = tiles // cap
    lane = lax.div(iota((1, tiles), 1), cap)

    def came_in(sources):
        first = sources[0] // per
        spans = range(first, sources[-1] // per + 1)
        hits = []
        for kind in range(2):
            parts = []
            for h in spans:
                pos = jnp.zeros((1, tiles), F32)
                for s in range(per):
                    if h * per + s in sources:
                        pos = jnp.where(lane == s, meta_in[h * per + s, kind : kind + 1, :], pos)
                pos = jnp.broadcast_to(pos.astype(I32), (tiles, tiles))
                parts.append(onehot(pos == iota((tiles, tiles), 0) + 1))
            hits.append(jnp.concatenate(parts, axis=1))
        number = iota((rows_e, len(spans) * tiles), 1) + (first * tiles + 1)
        return minor_dot(number.astype(F32).astype(BF16), jnp.concatenate(hits, axis=0)).astype(I32)

    def find(index, table):
        slot = lanes_of(table, lax.div(index, blocks))
        part = lax.rem(index, blocks)
        there = jnp.maximum(slot - 1, 0)
        vector = lax.div(there, cap) * vectors + lax.div(part, groups)
        return lax.rem(part, groups) * cap + lax.rem(there, cap), jnp.where(slot > 0, vector, -1)

    def find_all(sources):
        table = came_in(sources)
        return find(block[...], table[:, :tiles]) + find(other, table[:, tiles:])

    def spread(x, r):
        return jnp.broadcast_to(x[r : r + 1, :], (quad, tiles))

    def take(r, lane_at, vector_at, base, first, end, got):
        index, vector = spread(lane_at, r), spread(vector_at, r)

        def step(s, got):
            for v in range(vectors):
                low = base + v * quad
                here = lanes_of(inbox[s, low : low + quad, :], index)
                got = jnp.where(vector == s * vectors + v, here, got)
            return got

        return lax.fori_loop(first, end, step, got, unroll=end - first <= 16)

    def take_all(found, first, end, mine, theirs):
        for r in range(rows_e):
            mine[r] = take(r, found[0], found[1], 0, first, end, mine[r])
            theirs[r] = take(r, found[2], found[3], vectors * quad, first, end, theirs[r])

    def arrived(a, b, sent, got, sources):
        ours = (me >= sources[0]) & (me <= sources[-1])
        for many, there in ((len(sources) - 1, ours), (len(sources), jnp.logical_not(ours))):
            if many:

                @pl.when(there)
                def _():
                    several(a, b, many, sent, got).wait_recv()

    mine = [jnp.zeros((quad, tiles), F32)] * rows_e
    theirs = [jnp.zeros((quad, tiles), F32)] * rows_e
    arrived(meta_out, meta_in, 0, 4, parts_of[0])
    found = find_all(parts_of[0])
    for i, sources in enumerate(parts_of):
        arrived(outbox, inbox, 1, 4 + count + i, sources)
        if i + 1 < count:
            arrived(meta_out, meta_in, 0, 5 + i, parts_of[i + 1])
        take_all(found, sources[0], sources[-1] + 1, mine, theirs)
        if i + 1 < count:
            found = find_all(parts_of[i + 1])
    for r in range(rows_e):
        out[:, r * tiles : (r + 1) * tiles] = jnp.where(
            spread(shared, r) > 0, 0.5 * (mine[r] + theirs[r]), mine[r]
        )

    ghosts.wait_send()
    several(meta_out, meta_in, last, 0, 4).wait_send()
    several(outbox, inbox, last, 1, 4 + count).wait_send()


def per_device(tension, tile_dest, restriction, elem_block, shared_own, shared_send):
    n = lax.axis_size("ep")
    tiles = tension.shape[0]
    quad, nodes = restriction.shape
    vectors = layout(n, tiles, tension.shape[1], nodes)[3]
    halves = shared_own.shape[0] // tiles
    given = (
        tile_dest.reshape(1, tiles),
        shared_send.reshape(halves, tiles),
        elem_block.reshape(-1, tiles),
        restriction,
        shared_own.reshape(halves, tiles),
        tension,
    )
    return pl.pallas_call(
        functools.partial(kernel, n),
        out_shape=jax.ShapeDtypeStruct((quad, elem_block.shape[0]), F32),
        in_specs=[pl.BlockSpec(memory_space=pltpu.HBM)] * 6,
        out_specs=pl.BlockSpec(memory_space=pltpu.VMEM),
        scratch_shapes=[pltpu.VMEM(a.shape, a.dtype) for a in given]
        + [
            pltpu.VMEM((n, 2 * vectors * quad, tiles), F32),
            pltpu.VMEM((n, 2 * vectors * quad, tiles), F32),
            pltpu.VMEM((n, 2, tiles), F32),
            pltpu.VMEM((n, 2, tiles), F32),
            pltpu.VMEM((halves, tiles), I32),
            pltpu.VMEM((halves, tiles), I32),
            pltpu.SemaphoreType.DMA((6,)),
            pltpu.SemaphoreType.DMA((4 + 2 * (len(stages(n)) + 1),)),
            pltpu.SemaphoreType.REGULAR((n,)),
        ],
        compiler_params=pltpu.CompilerParams(
            collective_id=0, has_side_effects=True, vmem_limit_bytes=16 * 2**20
        ),
    )(*[pltpu.with_memory_space_constraint(a, pltpu.HBM) for a in given])


def solution(mesh):
    return jax.shard_map(
        per_device,
        mesh=mesh,
        in_specs=(
            P(("rep", "ep"), None),
            P(("rep", "ep")),
            P(),
            P(("rep", "ep")),
            P(("rep", "ep")),
            P(("rep", "ep")),
        ),
        out_specs=P(None, ("rep", "ep")),
        check_vma=False,
    )
```

```python
import functools

import jax
import jax.numpy as jnp
from jax import lax
from jax.experimental import pallas as pl
from jax.experimental.pallas import tpu as pltpu
from jax.sharding import PartitionSpec as P

F32 = jnp.float32
BF16 = jnp.bfloat16
I32 = jnp.int32
MINOR = (((1,), (1,)), ((), ()))
DEPTH = 256
ALONG_LANES = lax.GatherDimensionNumbers(
    offset_dims=(),
    collapsed_slice_dims=(1,),
    start_index_map=(1,),
    operand_batching_dims=(0,),
    start_indices_batching_dims=(0,),
)
LOADS = 4
HOLD = 1500


def iota(shape, dim):
    return lax.broadcasted_iota(I32, shape, dim)


def pieces(x):
    high = x.astype(BF16)
    return high, (x - high.astype(F32)).astype(BF16)


def onehot(x):
    return x.astype(F32).astype(BF16)


def minor_dot(a, b):
    return lax.dot_general(a, b, MINOR, preferred_element_type=F32)


def lanes_of(x, index):
    return lax.gather(
        x, index[..., None], ALONG_LANES, (1, 1), mode=lax.GatherScatterMode.PROMISE_IN_BOUNDS
    )


def layout(n, tiles, nodal, nodes):
    cap = 2 * tiles // n
    blocks = nodal // nodes
    groups = min(tiles // cap, blocks)
    return cap, blocks, groups, blocks // groups


def stages(n):
    return (n // 2 + 1, n - 1)


def kernel(n, *refs):
    given, out, held = refs[:6], refs[6], refs[7:13]
    outbox, inbox, meta_out, meta_in, ghost_out, ghost_in, load_sem, pair_sem, entered = refs[13:]
    dest, send, block, restriction, own, tension = held
    me = lax.axis_index("ep")
    tiles = tension.shape[0]
    quad, nodes = restriction.shape
    cap, blocks, groups, vectors = layout(n, tiles, tension.shape[1], nodes)
    rows_e = block.shape[0]
    halves = own.shape[0]
    wide = tiles * halves
    slots = n * cap
    cuts = tension.shape[1] // DEPTH

    small = [pltpu.make_async_copy(a, b, load_sem.at[i]) for i, (a, b) in enumerate(zip(given[:5], held[:5]))]
    rows = tiles // LOADS
    pieces_of = [pl.ds(c * rows, rows) for c in range(LOADS)]
    columns = [pltpu.make_async_copy(given[5].at[c], tension.at[c], load_sem.at[5]) for c in pieces_of]
    for load in small[:1] + small[3:4] + columns + small[1:3] + small[4:]:
        load.start()

    barrier = pltpu.get_barrier_semaphore()

    def each(first, last, step):
        lax.fori_loop(first, last, lambda p, _: (step(p), 0)[1], 0)

    each(me + 1, n, lambda p: pl.semaphore_signal(barrier, inc=1, device_id={"ep": p}))

    last = n - 1
    edges = stages(n)
    parts_of = [range(a, b) for a, b in zip((0,) + edges, edges + (n,))]
    count = len(parts_of)
    my_part = sum((me >= edge).astype(I32) for edge in edges)

    def remote(src, dst, sent, got, peer):
        return pltpu.make_async_remote_copy(
            src_ref=src, dst_ref=dst, send_sem=pair_sem.at[sent], recv_sem=pair_sem.at[got], device_id={"ep": peer}
        )

    def send_meta(p):
        remote(meta_out.at[p], meta_in.at[me], 0, 4 + my_part, p).start()

    def send_data(p):
        remote(outbox.at[p], inbox.at[me], 1, 4 + count + my_part, p).start()

    def send_both(p):
        send_meta(p)
        send_data(p)

    def several(a, b, many, sent, got):
        return remote(a.at[pl.ds(0, many)], b.at[pl.ds(0, many)], sent, got, lax.rem(me + 1, n))

    ghosts = remote(ghost_out, ghost_in, 2, 3, lax.rem(me + last, n))

    small[0].wait()
    small[3].wait()
    place = dest[...]
    target = lax.div(place, tiles)
    to_peer = (jnp.broadcast_to(target, (n, tiles)) == iota((n, tiles), 0)).astype(F32)
    earlier = onehot(iota((tiles, tiles), 0) < iota((tiles, tiles), 1))
    before = jnp.dot(to_peer.astype(BF16), earlier, preferred_element_type=F32)
    rank = jnp.sum(before * to_peer, axis=0, keepdims=True).astype(I32)
    at_rank = onehot(jnp.broadcast_to(rank, (tiles, tiles)) == lax.rem(iota((tiles, tiles), 0), cap))
    position = (lax.rem(place, tiles) + 1).astype(F32)
    wanted = jnp.concatenate([to_peer * iota((n, tiles), 1).astype(F32), to_peer * position], axis=0)
    wanted = minor_dot(wanted.astype(BF16), at_rank)
    tile_of, where_to = wanted[:n].astype(I32), wanted[n:]
    for p in range(n):
        meta_out[p, 0:1, :] = where_to[p : p + 1]
        meta_out[(p + n - 1) % n, 1:2, :] = where_to[p : p + 1]

    full = (DEPTH // nodes * quad, DEPTH)
    weight = jnp.concatenate([restriction[...]] * (DEPTH // nodes), axis=1)
    weight = jnp.concatenate([weight] * (DEPTH // nodes), axis=0)
    weight = jnp.where(lax.div(iota(full, 0), quad) == lax.div(iota(full, 1), nodes), weight, 0.0)
    weight = jnp.concatenate(pieces(weight), axis=0)

    @pl.when(me > 0)
    def _():
        pl.semaphore_wait(barrier, me)
        send_meta(0)

    pltpu.make_async_copy(given[5], tension, load_sem.at[5]).wait()
    local = []
    for c in range(cuts):
        high, low = pieces(tension[:, c * DEPTH : (c + 1) * DEPTH])
        part = minor_dot(weight, high)
        local.append(part[: full[0]] + (part[full[0] :] + minor_dot(weight[: full[0]], low)))
    local = jnp.concatenate(local, axis=0)
    group = lax.div(iota((quad, tiles), 1), cap)

    def pack(p):
        index = jnp.broadcast_to(tile_of[p : p + 1], (quad, tiles))
        for v in range(vectors):
            low = v * groups * quad
            got = lanes_of(local[low : low + quad], index)
            for g in range(1, groups):
                low = (v * groups + g) * quad
                got = jnp.where(group == g, lanes_of(local[low : low + quad], index), got)
            outbox[p, v * quad : (v + 1) * quad, :] = got
            outbox[(p + n - 1) % n, (vectors + v) * quad : (vectors + v + 1) * quad, :] = got

    pack(0)
    pack(1)

    @pl.when(me > 0)
    def _():
        send_data(0)

    small[1].wait()
    small[2].wait()
    each(0, me, lambda p: pl.semaphore_signal(entered.at[me], inc=1, device_id={"ep": p}))
    for h in range(halves):
        want = jnp.broadcast_to(send[h : h + 1, :], (rows_e, tiles))
        got = lanes_of(block[...], lax.rem(want, tiles))
        ghost_out[h : h + 1, :] = jnp.sum(
            jnp.where(lax.div(want, tiles) == iota((rows_e, tiles), 0), got, 0), axis=0, keepdims=True
        )

    @pl.when(me > 0)
    def _():
        ghosts.start()

    for p in range(2, n):
        pack(p)

    @pl.when(lax.rem(lax.axis_index("rep"), 2) == 1)
    def _():
        pl.delay(HOLD)

    each(1, me, send_both)

    def up(p):
        pl.semaphore_wait(entered.at[p], 1)
        send_both(p)

    each(me + 1, n, up)

    @pl.when(me == 0)
    def _():
        ghosts.start()

    meta_in[me] = meta_out[me]
    inbox[me] = outbox[me]

    small[4].wait()
    owned = jnp.concatenate([own[h : h + 1, :] for h in range(halves)], axis=1)
    entry = (iota((rows_e, wide), 1) + 1).astype(F32)
    entry = jnp.where(
        jnp.broadcast_to(lax.div(owned, tiles), (rows_e, wide)) == iota((rows_e, wide), 0), entry, 0.0
    ).astype(BF16)
    column = jnp.broadcast_to(lax.rem(owned, tiles), (tiles, wide)) == iota((tiles, wide), 0)
    shared = minor_dot(entry, onehot(column)).astype(I32)

    which = jnp.maximum(shared - 1, 0)
    ghosts.wait_recv()
    other = jnp.zeros((rows_e, tiles), I32)
    for h in range(halves):
        row = jnp.broadcast_to(ghost_in[h : h + 1, :], (rows_e, tiles))
        other = jnp.where(lax.div(which, tiles) == h, lanes_of(row, lax.rem(which, tiles)), other)

    per = tiles // cap
    lane = lax.div(iota((1, tiles), 1), cap)

    def came_in(sources):
        first = sources[0] // per
        spans = range(first, sources[-1] // per + 1)
        hits = []
        for kind in range(2):
            parts = []
            for h in spans:
                pos = jnp.zeros((1, tiles), F32)
                for s in range(per):
                    if h * per + s in sources:
                        pos = jnp.where(lane == s, meta_in[h * per + s, kind : kind + 1, :], pos)
                pos = jnp.broadcast_to(pos.astype(I32), (tiles, tiles))
                parts.append(onehot(pos == iota((tiles, tiles), 0) + 1))
            hits.append(jnp.concatenate(parts, axis=1))
        number = iota((rows_e, len(spans) * tiles), 1) + (first * tiles + 1)
        return minor_dot(number.astype(F32).astype(BF16), jnp.concatenate(hits, axis=0)).astype(I32)

    def find(index, table):
        slot = lanes_of(table, lax.div(index, blocks))
        part = lax.rem(index, blocks)
        there = jnp.maximum(slot - 1, 0)
        vector = lax.div(there, cap) * vectors + lax.div(part, groups)
        return lax.rem(part, groups) * cap + lax.rem(there, cap), jnp.where(slot > 0, vector, -1)

    def find_all(sources):
        table = came_in(sources)
        return find(block[...], table[:, :tiles]) + find(other, table[:, tiles:])

    def spread(x, r):
        return jnp.broadcast_to(x[r : r + 1, :], (quad, tiles))

    def take(r, lane_at, vector_at, base, first, end, got):
        index, vector = spread(lane_at, r), spread(vector_at, r)

        def step(s, got):
            for v in range(vectors):
                low = base + v * quad
                here = lanes_of(inbox[s, low : low + quad, :], index)
                got = jnp.where(vector == s * vectors + v, here, got)
            return got

        return lax.fori_loop(first, end, step, got, unroll=end - first <= 16)

    def take_all(found, first, end, mine, theirs):
        for r in range(rows_e):
            mine[r] = take(r, found[0], found[1], 0, first, end, mine[r])
            theirs[r] = take(r, found[2], found[3], vectors * quad, first, end, theirs[r])

    def arrived(a, b, sent, got, sources):
        ours = (me >= sources[0]) & (me <= sources[-1])
        for many, there in ((len(sources) - 1, ours), (len(sources), jnp.logical_not(ours))):
            if many:

                @pl.when(there)
                def _():
                    several(a, b, many, sent, got).wait_recv()

    mine = [jnp.zeros((quad, tiles), F32)] * rows_e
    theirs = [jnp.zeros((quad, tiles), F32)] * rows_e
    arrived(meta_out, meta_in, 0, 4, parts_of[0])
    found = find_all(parts_of[0])
    for i, sources in enumerate(parts_of):
        arrived(outbox, inbox, 1, 4 + count + i, sources)
        if i + 1 < count:
            arrived(meta_out, meta_in, 0, 5 + i, parts_of[i + 1])
        take_all(found, sources[0], sources[-1] + 1, mine, theirs)
        if i + 1 < count:
            found = find_all(parts_of[i + 1])
    for r in range(rows_e):
        out[:, r * tiles : (r + 1) * tiles] = jnp.where(
            spread(shared, r) > 0, 0.5 * (mine[r] + theirs[r]), mine[r]
        )

    ghosts.wait_send()
    several(meta_out, meta_in, last, 0, 4).wait_send()
    several(outbox, inbox, last, 1, 4 + count).wait_send()


def per_device(tension, tile_dest, restriction, elem_block, shared_own, shared_send):
    n = lax.axis_size("ep")
    tiles = tension.shape[0]
    quad, nodes = restriction.shape
    vectors = layout(n, tiles, tension.shape[1], nodes)[3]
    halves = shared_own.shape[0] // tiles
    given = (
        tile_dest.reshape(1, tiles),
        shared_send.reshape(halves, tiles),
        elem_block.reshape(-1, tiles),
        restriction,
        shared_own.reshape(halves, tiles),
        tension,
    )
    return pl.pallas_call(
        functools.partial(kernel, n),
        out_shape=jax.ShapeDtypeStruct((quad, elem_block.shape[0]), F32),
        in_specs=[pl.BlockSpec(memory_space=pltpu.HBM)] * 6,
        out_specs=pl.BlockSpec(memory_space=pltpu.VMEM),
        scratch_shapes=[pltpu.VMEM(a.shape, a.dtype) for a in given]
        + [
            pltpu.VMEM((n, 2 * vectors * quad, tiles), F32),
            pltpu.VMEM((n, 2 * vectors * quad, tiles), F32),
            pltpu.VMEM((n, 2, tiles), F32),
            pltpu.VMEM((n, 2, tiles), F32),
            pltpu.VMEM((halves, tiles), I32),
            pltpu.VMEM((halves, tiles), I32),
            pltpu.SemaphoreType.DMA((6,)),
            pltpu.SemaphoreType.DMA((4 + 2 * (len(stages(n)) + 1),)),
            pltpu.SemaphoreType.REGULAR((n,)),
        ],
        compiler_params=pltpu.CompilerParams(
            collective_id=0, has_side_effects=True, vmem_limit_bytes=16 * 2**20
        ),
    )(*[pltpu.with_memory_space_constraint(a, pltpu.HBM) for a in given])


def solution(mesh):
    return jax.shard_map(
        per_device,
        mesh=mesh,
        in_specs=(
            P(("rep", "ep"), None),
            P(("rep", "ep")),
            P(),
            P(("rep", "ep")),
            P(("rep", "ep")),
            P(("rep", "ep")),
        ),
        out_specs=P(None, ("rep", "ep")),
        check_vma=False,
    )
```

```python
import functools

import jax
import jax.numpy as jnp
from jax import lax
from jax.experimental import pallas as pl
from jax.experimental.pallas import tpu as pltpu
from jax.sharding import PartitionSpec as P

F32 = jnp.float32
BF16 = jnp.bfloat16
I32 = jnp.int32
MINOR = (((1,), (1,)), ((), ()))
DEPTH = 256
ALONG_LANES = lax.GatherDimensionNumbers(
    offset_dims=(),
    collapsed_slice_dims=(1,),
    start_index_map=(1,),
    operand_batching_dims=(0,),
    start_indices_batching_dims=(0,),
)
LOADS = 4
HOLD = 2200


def iota(shape, dim):
    return lax.broadcasted_iota(I32, shape, dim)


def pieces(x):
    high = x.astype(BF16)
    return high, (x - high.astype(F32)).astype(BF16)


def onehot(x):
    return x.astype(F32).astype(BF16)


def minor_dot(a, b):
    return lax.dot_general(a, b, MINOR, preferred_element_type=F32)


def lanes_of(x, index):
    return lax.gather(
        x, index[..., None], ALONG_LANES, (1, 1), mode=lax.GatherScatterMode.PROMISE_IN_BOUNDS
    )


def layout(n, tiles, nodal, nodes):
    cap = 2 * tiles // n
    blocks = nodal // nodes
    groups = min(tiles // cap, blocks)
    return cap, blocks, groups, blocks // groups


def stages(n):
    return (n // 2 + 1, n - 1)


def kernel(n, *refs):
    given, out, held = refs[:6], refs[6], refs[7:13]
    outbox, inbox, meta_out, meta_in, ghost_out, ghost_in, load_sem, pair_sem, entered = refs[13:]
    dest, send, block, restriction, own, tension = held
    me = lax.axis_index("ep")
    tiles = tension.shape[0]
    quad, nodes = restriction.shape
    cap, blocks, groups, vectors = layout(n, tiles, tension.shape[1], nodes)
    rows_e = block.shape[0]
    halves = own.shape[0]
    wide = tiles * halves
    slots = n * cap
    cuts = tension.shape[1] // DEPTH

    small = [pltpu.make_async_copy(a, b, load_sem.at[i]) for i, (a, b) in enumerate(zip(given[:5], held[:5]))]
    rows = tiles // LOADS
    pieces_of = [pl.ds(c * rows, rows) for c in range(LOADS)]
    columns = [pltpu.make_async_copy(given[5].at[c], tension.at[c], load_sem.at[5]) for c in pieces_of]
    for load in small[:1] + small[3:4] + columns + small[1:3] + small[4:]:
        load.start()

    barrier = pltpu.get_barrier_semaphore()

    def each(first, last, step):
        lax.fori_loop(first, last, lambda p, _: (step(p), 0)[1], 0)

    each(me + 1, n, lambda p: pl.semaphore_signal(barrier, inc=1, device_id={"ep": p}))

    last = n - 1
    edges = stages(n)
    parts_of = [range(a, b) for a, b in zip((0,) + edges, edges + (n,))]
    count = len(parts_of)
    my_part = sum((me >= edge).astype(I32) for edge in edges)

    def remote(src, dst, sent, got, peer):
        return pltpu.make_async_remote_copy(
            src_ref=src, dst_ref=dst, send_sem=pair_sem.at[sent], recv_sem=pair_sem.at[got], device_id={"ep": peer}
        )

    def send_meta(p):
        remote(meta_out.at[p], meta_in.at[me], 0, 4 + my_part, p).start()

    def send_data(p):
        remote(outbox.at[p], inbox.at[me], 1, 4 + count + my_part, p).start()

    def send_both(p):
        send_meta(p)
        send_data(p)

    def several(a, b, many, sent, got):
        return remote(a.at[pl.ds(0, many)], b.at[pl.ds(0, many)], sent, got, lax.rem(me + 1, n))

    ghosts = remote(ghost_out, ghost_in, 2, 3, lax.rem(me + last, n))

    small[0].wait()
    small[3].wait()
    place = dest[...]
    target = lax.div(place, tiles)
    to_peer = (jnp.broadcast_to(target, (n, tiles)) == iota((n, tiles), 0)).astype(F32)
    earlier = onehot(iota((tiles, tiles), 0) < iota((tiles, tiles), 1))
    before = jnp.dot(to_peer.astype(BF16), earlier, preferred_element_type=F32)
    rank = jnp.sum(before * to_peer, axis=0, keepdims=True).astype(I32)
    at_rank = onehot(jnp.broadcast_to(rank, (tiles, tiles)) == lax.rem(iota((tiles, tiles), 0), cap))
    position = (lax.rem(place, tiles) + 1).astype(F32)
    wanted = jnp.concatenate([to_peer * iota((n, tiles), 1).astype(F32), to_peer * position], axis=0)
    wanted = minor_dot(wanted.astype(BF16), at_rank)
    tile_of, where_to = wanted[:n].astype(I32), wanted[n:]
    for p in range(n):
        meta_out[p, 0:1, :] = where_to[p : p + 1]
        meta_out[(p + n - 1) % n, 1:2, :] = where_to[p : p + 1]

    full = (DEPTH // nodes * quad, DEPTH)
    weight = jnp.concatenate([restriction[...]] * (DEPTH // nodes), axis=1)
    weight = jnp.concatenate([weight] * (DEPTH // nodes), axis=0)
    weight = jnp.where(lax.div(iota(full, 0), quad) == lax.div(iota(full, 1), nodes), weight, 0.0)
    weight = jnp.concatenate(pieces(weight), axis=0)

    @pl.when(me > 0)
    def _():
        pl.semaphore_wait(barrier, me)
        send_meta(0)

    pltpu.make_async_copy(given[5], tension, load_sem.at[5]).wait()
    local = []
    for c in range(cuts):
        high, low = pieces(tension[:, c * DEPTH : (c + 1) * DEPTH])
        part = minor_dot(weight, high)
        local.append(part[: full[0]] + (part[full[0] :] + minor_dot(weight[: full[0]], low)))
    local = jnp.concatenate(local, axis=0)
    group = lax.div(iota((quad, tiles), 1), cap)

    def pack(p):
        index = jnp.broadcast_to(tile_of[p : p + 1], (quad, tiles))
        for v in range(vectors):
            low = v * groups * quad
            got = lanes_of(local[low : low + quad], index)
            for g in range(1, groups):
                low = (v * groups + g) * quad
                got = jnp.where(group == g, lanes_of(local[low : low + quad], index), got)
            outbox[p, v * quad : (v + 1) * quad, :] = got
            outbox[(p + n - 1) % n, (vectors + v) * quad : (vectors + v + 1) * quad, :] = got

    pack(0)
    pack(1)

    @pl.when(me > 0)
    def _():
        send_data(0)

    small[1].wait()
    small[2].wait()
    each(0, me, lambda p: pl.semaphore_signal(entered.at[me], inc=1, device_id={"ep": p}))
    for h in range(halves):
        want = jnp.broadcast_to(send[h : h + 1, :], (rows_e, tiles))
        got = lanes_of(block[...], lax.rem(want, tiles))
        ghost_out[h : h + 1, :] = jnp.sum(
            jnp.where(lax.div(want, tiles) == iota((rows_e, tiles), 0), got, 0), axis=0, keepdims=True
        )

    @pl.when(me > 0)
    def _():
        ghosts.start()

    for p in range(2, n):
        pack(p)

    @pl.when(lax.rem(lax.axis_index("rep"), 2) == 1)
    def _():
        pl.delay(HOLD)

    each(1, me, send_both)

    def up(p):
        pl.semaphore_wait(entered.at[p], 1)
        send_both(p)

    each(me + 1, n, up)

    @pl.when(me == 0)
    def _():
        ghosts.start()

    meta_in[me] = meta_out[me]
    inbox[me] = outbox[me]

    small[4].wait()
    owned = jnp.concatenate([own[h : h + 1, :] for h in range(halves)], axis=1)
    entry = (iota((rows_e, wide), 1) + 1).astype(F32)
    entry = jnp.where(
        jnp.broadcast_to(lax.div(owned, tiles), (rows_e, wide)) == iota((rows_e, wide), 0), entry, 0.0
    ).astype(BF16)
    column = jnp.broadcast_to(lax.rem(owned, tiles), (tiles, wide)) == iota((tiles, wide), 0)
    shared = minor_dot(entry, onehot(column)).astype(I32)

    which = jnp.maximum(shared - 1, 0)
    ghosts.wait_recv()
    other = jnp.zeros((rows_e, tiles), I32)
    for h in range(halves):
        row = jnp.broadcast_to(ghost_in[h : h + 1, :], (rows_e, tiles))
        other = jnp.where(lax.div(which, tiles) == h, lanes_of(row, lax.rem(which, tiles)), other)

    per = tiles // cap
    lane = lax.div(iota((1, tiles), 1), cap)

    def came_in(sources):
        first = sources[0] // per
        spans = range(first, sources[-1] // per + 1)
        hits = []
        for kind in range(2):
            parts = []
            for h in spans:
                pos = jnp.zeros((1, tiles), F32)
                for s in range(per):
                    if h * per + s in sources:
                        pos = jnp.where(lane == s, meta_in[h * per + s, kind : kind + 1, :], pos)
                pos = jnp.broadcast_to(pos.astype(I32), (tiles, tiles))
                parts.append(onehot(pos == iota((tiles, tiles), 0) + 1))
            hits.append(jnp.concatenate(parts, axis=1))
        number = iota((rows_e, len(spans) * tiles), 1) + (first * tiles + 1)
        return minor_dot(number.astype(F32).astype(BF16), jnp.concatenate(hits, axis=0)).astype(I32)

    def find(index, table):
        slot = lanes_of(table, lax.div(index, blocks))
        part = lax.rem(index, blocks)
        there = jnp.maximum(slot - 1, 0)
        vector = lax.div(there, cap) * vectors + lax.div(part, groups)
        return lax.rem(part, groups) * cap + lax.rem(there, cap), jnp.where(slot > 0, vector, -1)

    def find_all(sources):
        table = came_in(sources)
        return find(block[...], table[:, :tiles]) + find(other, table[:, tiles:])

    def spread(x, r):
        return jnp.broadcast_to(x[r : r + 1, :], (quad, tiles))

    def take(r, lane_at, vector_at, base, first, end, got):
        index, vector = spread(lane_at, r), spread(vector_at, r)

        def step(s, got):
            for v in range(vectors):
                low = base + v * quad
                here = lanes_of(inbox[s, low : low + quad, :], index)
                got = jnp.where(vector == s * vectors + v, here, got)
            return got

        return lax.fori_loop(first, end, step, got, unroll=end - first <= 16)

    def take_all(found, first, end, mine, theirs):
        for r in range(rows_e):
            mine[r] = take(r, found[0], found[1], 0, first, end, mine[r])
            theirs[r] = take(r, found[2], found[3], vectors * quad, first, end, theirs[r])

    def arrived(a, b, sent, got, sources):
        ours = (me >= sources[0]) & (me <= sources[-1])
        for many, there in ((len(sources) - 1, ours), (len(sources), jnp.logical_not(ours))):
            if many:

                @pl.when(there)
                def _():
                    several(a, b, many, sent, got).wait_recv()

    mine = [jnp.zeros((quad, tiles), F32)] * rows_e
    theirs = [jnp.zeros((quad, tiles), F32)] * rows_e
    arrived(meta_out, meta_in, 0, 4, parts_of[0])
    found = find_all(parts_of[0])
    for i, sources in enumerate(parts_of):
        arrived(outbox, inbox, 1, 4 + count + i, sources)
        if i + 1 < count:
            arrived(meta_out, meta_in, 0, 5 + i, parts_of[i + 1])
        take_all(found, sources[0], sources[-1] + 1, mine, theirs)
        if i + 1 < count:
            found = find_all(parts_of[i + 1])
    for r in range(rows_e):
        out[:, r * tiles : (r + 1) * tiles] = jnp.where(
            spread(shared, r) > 0, 0.5 * (mine[r] + theirs[r]), mine[r]
        )

    ghosts.wait_send()
    several(meta_out, meta_in, last, 0, 4).wait_send()
    several(outbox, inbox, last, 1, 4 + count).wait_send()


def per_device(tension, tile_dest, restriction, elem_block, shared_own, shared_send):
    n = lax.axis_size("ep")
    tiles = tension.shape[0]
    quad, nodes = restriction.shape
    vectors = layout(n, tiles, tension.shape[1], nodes)[3]
    halves = shared_own.shape[0] // tiles
    given = (
        tile_dest.reshape(1, tiles),
        shared_send.reshape(halves, tiles),
        elem_block.reshape(-1, tiles),
        restriction,
        shared_own.reshape(halves, tiles),
        tension,
    )
    return pl.pallas_call(
        functools.partial(kernel, n),
        out_shape=jax.ShapeDtypeStruct((quad, elem_block.shape[0]), F32),
        in_specs=[pl.BlockSpec(memory_space=pltpu.HBM)] * 6,
        out_specs=pl.BlockSpec(memory_space=pltpu.VMEM),
        scratch_shapes=[pltpu.VMEM(a.shape, a.dtype) for a in given]
        + [
            pltpu.VMEM((n, 2 * vectors * quad, tiles), F32),
            pltpu.VMEM((n, 2 * vectors * quad, tiles), F32),
            pltpu.VMEM((n, 2, tiles), F32),
            pltpu.VMEM((n, 2, tiles), F32),
            pltpu.VMEM((halves, tiles), I32),
            pltpu.VMEM((halves, tiles), I32),
            pltpu.SemaphoreType.DMA((6,)),
            pltpu.SemaphoreType.DMA((4 + 2 * (len(stages(n)) + 1),)),
            pltpu.SemaphoreType.REGULAR((n,)),
        ],
        compiler_params=pltpu.CompilerParams(
            collective_id=0, has_side_effects=True, vmem_limit_bytes=16 * 2**20
        ),
    )(*[pltpu.with_memory_space_constraint(a, pltpu.HBM) for a in given])


def solution(mesh):
    return jax.shard_map(
        per_device,
        mesh=mesh,
        in_specs=(
            P(("rep", "ep"), None),
            P(("rep", "ep")),
            P(),
            P(("rep", "ep")),
            P(("rep", "ep")),
            P(("rep", "ep")),
        ),
        out_specs=P(None, ("rep", "ep")),
        check_vma=False,
    )
```

```python
import functools

import jax
import jax.numpy as jnp
from jax import lax
from jax.experimental import pallas as pl
from jax.experimental.pallas import tpu as pltpu
from jax.sharding import PartitionSpec as P

F32 = jnp.float32
BF16 = jnp.bfloat16
I32 = jnp.int32
MINOR = (((1,), (1,)), ((), ()))
DEPTH = 256
ALONG_LANES = lax.GatherDimensionNumbers(
    offset_dims=(),
    collapsed_slice_dims=(1,),
    start_index_map=(1,),
    operand_batching_dims=(0,),
    start_indices_batching_dims=(0,),
)
LOADS = 8
HOLD = 1500


def iota(shape, dim):
    return lax.broadcasted_iota(I32, shape, dim)


def pieces(x):
    high = x.astype(BF16)
    return high, (x - high.astype(F32)).astype(BF16)


def onehot(x):
    return x.astype(F32).astype(BF16)


def minor_dot(a, b):
    return lax.dot_general(a, b, MINOR, preferred_element_type=F32)


def lanes_of(x, index):
    return lax.gather(
        x, index[..., None], ALONG_LANES, (1, 1), mode=lax.GatherScatterMode.PROMISE_IN_BOUNDS
    )


def layout(n, tiles, nodal, nodes):
    cap = 2 * tiles // n
    blocks = nodal // nodes
    groups = min(tiles // cap, blocks)
    return cap, blocks, groups, blocks // groups


def stages(n):
    return (n - 2, n - 1)


def kernel(n, *refs):
    given, out, held = refs[:6], refs[6], refs[7:13]
    outbox, inbox, meta_out, meta_in, ghost_out, ghost_in, load_sem, pair_sem, entered = refs[13:]
    dest, send, block, restriction, own, tension = held
    me = lax.axis_index("ep")
    tiles = tension.shape[0]
    quad, nodes = restriction.shape
    cap, blocks, groups, vectors = layout(n, tiles, tension.shape[1], nodes)
    rows_e = block.shape[0]
    halves = own.shape[0]
    wide = tiles * halves
    slots = n * cap
    cuts = tension.shape[1] // DEPTH

    small = [pltpu.make_async_copy(a, b, load_sem.at[i]) for i, (a, b) in enumerate(zip(given[:5], held[:5]))]
    rows = tiles // LOADS
    pieces_of = [pl.ds(c * rows, rows) for c in range(LOADS)]
    columns = [pltpu.make_async_copy(given[5].at[c], tension.at[c], load_sem.at[5]) for c in pieces_of]
    for load in small[:1] + small[3:4] + columns + small[1:3] + small[4:]:
        load.start()

    barrier = pltpu.get_barrier_semaphore()

    def each(first, last, step):
        lax.fori_loop(first, last, lambda p, _: (step(p), 0)[1], 0)

    each(me + 1, n, lambda p: pl.semaphore_signal(barrier, inc=1, device_id={"ep": p}))

    last = n - 1
    edges = stages(n)
    parts_of = [range(a, b) for a, b in zip((0,) + edges, edges + (n,))]
    count = len(parts_of)
    my_part = sum((me >= edge).astype(I32) for edge in edges)

    def remote(src, dst, sent, got, peer):
        return pltpu.make_async_remote_copy(
            src_ref=src, dst_ref=dst, send_sem=pair_sem.at[sent], recv_sem=pair_sem.at[got], device_id={"ep": peer}
        )

    def send_meta(p):
        remote(meta_out.at[p], meta_in.at[me], 0, 4 + my_part, p).start()

    def send_data(p):
        remote(outbox.at[p], inbox.at[me], 1, 4 + count + my_part, p).start()

    def send_both(p):
        send_meta(p)
        send_data(p)

    def several(a, b, many, sent, got):
        return remote(a.at[pl.ds(0, many)], b.at[pl.ds(0, many)], sent, got, lax.rem(me + 1, n))

    ghosts = remote(ghost_out, ghost_in, 2, 3, lax.rem(me + last, n))

    small[0].wait()
    small[3].wait()
    place = dest[...]
    target = lax.div(place, tiles)
    to_peer = (jnp.broadcast_to(target, (n, tiles)) == iota((n, tiles), 0)).astype(F32)
    earlier = onehot(iota((tiles, tiles), 0) < iota((tiles, tiles), 1))
    before = jnp.dot(to_peer.astype(BF16), earlier, preferred_element_type=F32)
    rank = jnp.sum(before * to_peer, axis=0, keepdims=True).astype(I32)
    at_rank = onehot(jnp.broadcast_to(rank, (tiles, tiles)) == lax.rem(iota((tiles, tiles), 0), cap))
    position = (lax.rem(place, tiles) + 1).astype(F32)
    wanted = jnp.concatenate([to_peer * iota((n, tiles), 1).astype(F32), to_peer * position], axis=0)
    wanted = minor_dot(wanted.astype(BF16), at_rank)
    tile_of, where_to = wanted[:n].astype(I32), wanted[n:]
    for p in range(n):
        meta_out[p, 0:1, :] = where_to[p : p + 1]
        meta_out[(p + n - 1) % n, 1:2, :] = where_to[p : p + 1]

    full = (DEPTH // nodes * quad, DEPTH)
    weight = jnp.concatenate([restriction[...]] * (DEPTH // nodes), axis=1)
    weight = jnp.concatenate([weight] * (DEPTH // nodes), axis=0)
    weight = jnp.where(lax.div(iota(full, 0), quad) == lax.div(iota(full, 1), nodes), weight, 0.0)
    weight = jnp.concatenate(pieces(weight), axis=0)

    @pl.when(me > 0)
    def _():
        pl.semaphore_wait(barrier, me)
        send_meta(0)

    pltpu.make_async_copy(given[5], tension, load_sem.at[5]).wait()
    local = []
    for c in range(cuts):
        high, low = pieces(tension[:, c * DEPTH : (c + 1) * DEPTH])
        part = minor_dot(weight, high)
        local.append(part[: full[0]] + (part[full[0] :] + minor_dot(weight[: full[0]], low)))
    local = jnp.concatenate(local, axis=0)
    group = lax.div(iota((quad, tiles), 1), cap)

    def pack(p):
        index = jnp.broadcast_to(tile_of[p : p + 1], (quad, tiles))
        for v in range(vectors):
            low = v * groups * quad
            got = lanes_of(local[low : low + quad], index)
            for g in range(1, groups):
                low = (v * groups + g) * quad
                got = jnp.where(group == g, lanes_of(local[low : low + quad], index), got)
            outbox[p, v * quad : (v + 1) * quad, :] = got
            outbox[(p + n - 1) % n, (vectors + v) * quad : (vectors + v + 1) * quad, :] = got

    pack(0)
    pack(1)

    @pl.when(me > 0)
    def _():
        send_data(0)

    small[1].wait()
    small[2].wait()
    each(0, me, lambda p: pl.semaphore_signal(entered.at[me], inc=1, device_id={"ep": p}))
    for h in range(halves):
        want = jnp.broadcast_to(send[h : h + 1, :], (rows_e, tiles))
        got = lanes_of(block[...], lax.rem(want, tiles))
        ghost_out[h : h + 1, :] = jnp.sum(
            jnp.where(lax.div(want, tiles) == iota((rows_e, tiles), 0), got, 0), axis=0, keepdims=True
        )

    @pl.when(me > 0)
    def _():
        ghosts.start()

    for p in range(2, n):
        pack(p)

    @pl.when(lax.rem(lax.axis_index("rep"), 2) == 1)
    def _():
        pl.delay(HOLD)

    each(1, me, send_both)

    def up(p):
        pl.semaphore_wait(entered.at[p], 1)
        send_both(p)

    each(me + 1, n, up)

    @pl.when(me == 0)
    def _():
        ghosts.start()

    meta_in[me] = meta_out[me]
    inbox[me] = outbox[me]

    small[4].wait()
    owned = jnp.concatenate([own[h : h + 1, :] for h in range(halves)], axis=1)
    entry = (iota((rows_e, wide), 1) + 1).astype(F32)
    entry = jnp.where(
        jnp.broadcast_to(lax.div(owned, tiles), (rows_e, wide)) == iota((rows_e, wide), 0), entry, 0.0
    ).astype(BF16)
    column = jnp.broadcast_to(lax.rem(owned, tiles), (tiles, wide)) == iota((tiles, wide), 0)
    shared = minor_dot(entry, onehot(column)).astype(I32)

    which = jnp.maximum(shared - 1, 0)
    ghosts.wait_recv()
    other = jnp.zeros((rows_e, tiles), I32)
    for h in range(halves):
        row = jnp.broadcast_to(ghost_in[h : h + 1, :], (rows_e, tiles))
        other = jnp.where(lax.div(which, tiles) == h, lanes_of(row, lax.rem(which, tiles)), other)

    per = tiles // cap
    lane = lax.div(iota((1, tiles), 1), cap)

    def came_in(sources):
        first = sources[0] // per
        spans = range(first, sources[-1] // per + 1)
        hits = []
        for kind in range(2):
            parts = []
            for h in spans:
                pos = jnp.zeros((1, tiles), F32)
                for s in range(per):
                    if h * per + s in sources:
                        pos = jnp.where(lane == s, meta_in[h * per + s, kind : kind + 1, :], pos)
                pos = jnp.broadcast_to(pos.astype(I32), (tiles, tiles))
                parts.append(onehot(pos == iota((tiles, tiles), 0) + 1))
            hits.append(jnp.concatenate(parts, axis=1))
        number = iota((rows_e, len(spans) * tiles), 1) + (first * tiles + 1)
        return minor_dot(number.astype(F32).astype(BF16), jnp.concatenate(hits, axis=0)).astype(I32)

    def find(index, table):
        slot = lanes_of(table, lax.div(index, blocks))
        part = lax.rem(index, blocks)
        there = jnp.maximum(slot - 1, 0)
        vector = lax.div(there, cap) * vectors + lax.div(part, groups)
        return lax.rem(part, groups) * cap + lax.rem(there, cap), jnp.where(slot > 0, vector, -1)

    def find_all(sources):
        table = came_in(sources)
        return find(block[...], table[:, :tiles]) + find(other, table[:, tiles:])

    def spread(x, r):
        return jnp.broadcast_to(x[r : r + 1, :], (quad, tiles))

    def take(r, lane_at, vector_at, base, first, end, got):
        index, vector = spread(lane_at, r), spread(vector_at, r)

        def step(s, got):
            for v in range(vectors):
                low = base + v * quad
                here = lanes_of(inbox[s, low : low + quad, :], index)
                got = jnp.where(vector == s * vectors + v, here, got)
            return got

        return lax.fori_loop(first, end, step, got, unroll=end - first <= 16)

    def take_all(found, first, end, mine, theirs):
        for r in range(rows_e):
            mine[r] = take(r, found[0], found[1], 0, first, end, mine[r])
            theirs[r] = take(r, found[2], found[3], vectors * quad, first, end, theirs[r])

    def arrived(a, b, sent, got, sources):
        ours = (me >= sources[0]) & (me <= sources[-1])
        for many, there in ((len(sources) - 1, ours), (len(sources), jnp.logical_not(ours))):
            if many:

                @pl.when(there)
                def _():
                    several(a, b, many, sent, got).wait_recv()

    mine = [jnp.zeros((quad, tiles), F32)] * rows_e
    theirs = [jnp.zeros((quad, tiles), F32)] * rows_e
    arrived(meta_out, meta_in, 0, 4, parts_of[0])
    found = find_all(parts_of[0])
    for i, sources in enumerate(parts_of):
        arrived(outbox, inbox, 1, 4 + count + i, sources)
        if i + 1 < count:
            arrived(meta_out, meta_in, 0, 5 + i, parts_of[i + 1])
        take_all(found, sources[0], sources[-1] + 1, mine, theirs)
        if i + 1 < count:
            found = find_all(parts_of[i + 1])
    for r in range(rows_e):
        out[:, r * tiles : (r + 1) * tiles] = jnp.where(
            spread(shared, r) > 0, 0.5 * (mine[r] + theirs[r]), mine[r]
        )

    ghosts.wait_send()
    several(meta_out, meta_in, last, 0, 4).wait_send()
    several(outbox, inbox, last, 1, 4 + count).wait_send()


def per_device(tension, tile_dest, restriction, elem_block, shared_own, shared_send):
    n = lax.axis_size("ep")
    tiles = tension.shape[0]
    quad, nodes = restriction.shape
    vectors = layout(n, tiles, tension.shape[1], nodes)[3]
    halves = shared_own.shape[0] // tiles
    given = (
        tile_dest.reshape(1, tiles),
        shared_send.reshape(halves, tiles),
        elem_block.reshape(-1, tiles),
        restriction,
        shared_own.reshape(halves, tiles),
        tension,
    )
    return pl.pallas_call(
        functools.partial(kernel, n),
        out_shape=jax.ShapeDtypeStruct((quad, elem_block.shape[0]), F32),
        in_specs=[pl.BlockSpec(memory_space=pltpu.HBM)] * 6,
        out_specs=pl.BlockSpec(memory_space=pltpu.VMEM),
        scratch_shapes=[pltpu.VMEM(a.shape, a.dtype) for a in given]
        + [
            pltpu.VMEM((n, 2 * vectors * quad, tiles), F32),
            pltpu.VMEM((n, 2 * vectors * quad, tiles), F32),
            pltpu.VMEM((n, 2, tiles), F32),
            pltpu.VMEM((n, 2, tiles), F32),
            pltpu.VMEM((halves, tiles), I32),
            pltpu.VMEM((halves, tiles), I32),
            pltpu.SemaphoreType.DMA((6,)),
            pltpu.SemaphoreType.DMA((4 + 2 * (len(stages(n)) + 1),)),
            pltpu.SemaphoreType.REGULAR((n,)),
        ],
        compiler_params=pltpu.CompilerParams(
            collective_id=0, has_side_effects=True, vmem_limit_bytes=16 * 2**20
        ),
    )(*[pltpu.with_memory_space_constraint(a, pltpu.HBM) for a in given])


def solution(mesh):
    return jax.shard_map(
        per_device,
        mesh=mesh,
        in_specs=(
            P(("rep", "ep"), None),
            P(("rep", "ep")),
            P(),
            P(("rep", "ep")),
            P(("rep", "ep")),
            P(("rep", "ep")),
        ),
        out_specs=P(None, ("rep", "ep")),
        check_vma=False,
    )
```
